256 devices in a mesh: expert: 8 (over x, core), ffn: 32 (over z, y).
Axes of the slice: x: 4, y: 4, z: 8, core: 2. Of those that a mesh axis runs over, the one named last changes fastest.
Arguments:
- tokens: bfloat16 [8, 128, 4096], P('expert', 'ffn'), may hold values from -6 to 6
- routes: int32 [8, 128, 2], P('expert'), may hold values from 0 to 7, all different within a row; in each aligned block of 128 rows (0 to 127, 128 to 255, ..., all dimensions but the last counted through in order) at most 48 rows name the same one
- router: bfloat16 [4096, 8], replicated, may hold values from -0.09375 to 0.09375
- w_gate: bfloat16 [8, 4096, 12288], P('expert', None, 'ffn'), may hold values from -0.09375 to 0.09375
- w_up: bfloat16 [8, 4096, 12288], P('expert', None, 'ffn'), may hold values from -0.09375 to 0.09375
- w_down: bfloat16 [8, 12288, 4096], P('expert', 'ffn'), may hold values from -0.109375 to 0.109375
- adapter: bfloat16 [8, 4096, 4096], P('expert', None, 'ffn'), may hold values from -0.09375 to 0.09375
- upstream: bfloat16 [8, 128, 4096], P('expert', None, 'ffn'), may hold values from -24 to 24
- bound: float32 [8], P('expert'), may hold values from 2048 to 16384
Outputs:
- adapted: bfloat16 [8, 128, 4096], P('expert', None, 'ffn')
- clipped: bfloat16 [8, 4096, 4096], P('expert', None, 'ffn')
The draws below stay inside these ranges and needn't reach their ends.
Inputs may be any that keep to these rules, and one draw needn't show every extreme that they name: `routes`: each token names two different experts; for each client at most 48 of its tokens name any one expert, and in some clients some expert is named by exactly 48 tokens.
All inputs are finite; a program needn't handle non-finite values.
Results may differ from the reference program's by a relative error of at most 0.015.
Values may be sent and summed in bfloat16 or wider, within the bound.
No kernel may reach another device: no remote copies, remote signals or barrier semaphores. Data moves between devices by JAX's collectives and lax.ppermute only.
A program may use at most 64 MiB of HBM per device.

```python
import math
import jax
import jax.numpy as jnp
import numpy as np
from jax import lax

D = 4096
FF = 12288
EXPERTS = 8
CLIENTS = 8
TOK_CL = 128
CAP = 48
FF_DEV = 384
COLS_DEV = 128
N_FFN = 32


def draw_upstream(key, part):
    key_noise = jax.random.fold_in(key, 11)
    key_scale = jax.random.fold_in(key, 23)
    noise_part = jax.random.normal(key_noise, (CLIENTS, TOK_CL, D), jnp.float32)
    block_scales = jnp.exp(jax.random.uniform(key_scale, (CLIENTS, 1, D // COLS_DEV), jnp.float32, math.log(0.25), math.log(4.0)))
    scales = jnp.repeat(block_scales, COLS_DEV, axis=2)
    values = noise_part * scales
    return jnp.clip(values, -24.0, 24.0).astype(jnp.bfloat16)


def raised(array, own_key, source, target, blocks, factor):
    def block_of(position):
        return (jnp.arange(array.shape[position]) // (array.shape[position] // blocks)).reshape((-1,) + (1,) * (array.ndim - 1 - position))

    first = jax.random.permutation(own_key, blocks)[block_of(target)]
    far = (block_of(target) + blocks // 2) % blocks
    return jnp.where((block_of(source) == first) | (block_of(source) == far), factor * array, array)


def shard_levels(key, extent, cuts, smallest, largest):
    loudness = 1.0
    for position, parts in cuts:
        steps = jax.random.uniform(jax.random.fold_in(jax.random.fold_in(key, 6), position), (parts,), jnp.float32, smallest / len(cuts), largest / len(cuts))
        loudness = loudness * jnp.repeat(jnp.exp(steps), extent[position] // parts).reshape((-1,) + (1,) * (len(extent) - 1 - position))
    return loudness


def routed_block(key, own, number, rows, number_of, top, limit, lean):
    sequence = jax.random.permutation(key, number_of)
    crowded, ordinary = shares(number_of, rows * top, limit, lean, True), shares(number_of, rows * top, limit, lean, False)
    places = jnp.arange(number_of)

    def named(tallies, turn):
        used = int((tallies > 0).sum())
        fixed = max(1, used // 4)
        passed = fixed + (places - fixed + turn * (used - fixed)) % max(1, number_of - fixed)
        return jnp.zeros((number_of,), jnp.int32).at[sequence[jnp.where(places < fixed, places, passed)]].set(jnp.asarray(tallies, jnp.int32))

    tallies = jnp.where(number % 4 == 0, named(crowded, number // 4), named(ordinary, number - number // 4 - 1))
    mixed = jax.random.permutation(jax.random.fold_in(own, 3), number_of)
    donor, taker = mixed[0:number_of // 2 * 2:2], mixed[1:number_of // 2 * 2:2]
    slack = jnp.minimum(tallies[donor] - 1, limit - tallies[taker]) // 2
    slack = jnp.where((donor == sequence[0]) | (taker == sequence[0]) | (tallies[taker] == 0), 0, jnp.maximum(slack, 0))
    passed = jax.random.randint(jax.random.fold_in(own, 4), (number_of // 2,), 0, 1 << 20) % (slack + 1)
    tallies = tallies.at[donor].add(-passed).at[taker].add(passed)
    members = jnp.searchsorted(jnp.cumsum(tallies), jnp.arange(rows * top), side="right").astype(jnp.int32)
    grid = members.reshape(top, rows).T
    grid = grid[jax.random.permutation(jax.random.fold_in(own, 1), rows)]
    turn = jax.random.randint(jax.random.fold_in(own, 2), (rows, 1), 0, top)
    return jnp.take_along_axis(grid, (jnp.arange(top)[None, :] + turn) % top, axis=1)


def shares(amount, total, most, skew, full):
    loads = [(1 << 20) // math.isqrt(grade ** skew) + 1 for grade in range(1, amount + 1)]
    largest = most if full else min(most, max(-(-total // amount), total * loads[0] // sum(loads)))
    least = 1 if total - largest >= amount - 1 else 0
    counts, spare = [largest] + [least] * (amount - 1), total - largest - least * (amount - 1)
    while spare > 0:
        candidates = [i for i in range(1, amount) if counts[i] < largest] or [i for i in range(1, amount) if counts[i] < most]
        pool, left = sum([loads[i] for i in candidates]), spare
        for i in candidates:
            more = min(most - counts[i], max(1, left * loads[i] // pool), spare)
            counts[i] = counts[i] + more
            spare = spare - more
    return np.array(counts)


def noise(key, extent, scale, most, shards=(), held_as=jnp.bfloat16):
    array = jax.random.normal(key, extent, jnp.float32) * scale
    if len(shards) > 0:
        array = shard_levels(key, extent, shards, -0.22, 0.18) * array
    return jnp.clip(array, min=-most, max=most).astype(held_as)


def noise_with(key, dims, scale, limit, pieces, heavy, held_as=jnp.bfloat16):
    array = scale * jax.random.normal(key, dims, jnp.float32)
    if pieces:
        array = array * shard_levels(key, dims, pieces, -0.22, 0.18)
    return jnp.clip(raised(array, jax.random.fold_in(key, 3), *heavy), -limit, limit).astype(held_as)


def setup_inputs(seed: int = 0) -> dict:
    key_list = jax.random.split(jax.random.key(seed), 10)
    tokens = noise(key_list[0], (CLIENTS, TOK_CL, D), 1.0, 6.0, ((0, 8), (1, 32)))
    routes_keys = jax.random.split(jax.random.fold_in(key_list[1], 1), CLIENTS * TOK_CL // TOK_CL)
    routes_turns = jax.random.permutation(jax.random.fold_in(key_list[1], 3), CLIENTS * TOK_CL // TOK_CL)
    routes = jax.vmap(lambda own, number: routed_block(jax.random.fold_in(key_list[1], 2), own, number, TOK_CL, EXPERTS, 2, CAP, 1))(routes_keys, routes_turns).reshape((CLIENTS, TOK_CL, 2))
    router = noise(key_list[2], (D, EXPERTS), D ** -0.5, 0.09375)
    w_gate = noise(key_list[3], (EXPERTS, D, FF), D ** -0.5, 0.09375, ((0, 8), (2, 32)))
    w_up = noise(key_list[4], (EXPERTS, D, FF), D ** -0.5, 0.09375, ((0, 8), (2, 32)))
    w_down = noise_with(key_list[5], (EXPERTS, FF, D), FF ** -0.5, 0.109375, ((0, 8), (1, 32)), (1, 2, 32, 2.75))
    adapter = noise(key_list[6], (CLIENTS, D, D), D ** -0.5, 0.09375, ((0, 8), (2, 32)))
    upstream = draw_upstream(jax.random.fold_in(key_list[9], 71), 0)
    bound = jnp.clip(jnp.exp(math.log(16384.0) - 2.0794415 * jax.random.uniform(key_list[8], (CLIENTS,), jnp.float32) ** shard_levels(key_list[8], (CLIENTS,), ((0, 8),), -0.2, 0.2)), 2048.0, 16384.0)
    return {"tokens": tokens, "routes": routes, "router": router, "w_gate": w_gate, "w_up": w_up, "w_down": w_down, "adapter": adapter, "upstream": upstream, "bound": bound}


def slot_table(routed, expert_count):
    named_hits = lax.optimization_barrier(jnp.sum((routed[:, :, None] == jnp.arange(expert_count, dtype=jnp.int32)[None, None, :]).astype(jnp.int32), axis=1))
    before = jnp.cumsum(named_hits, axis=0) - named_hits
    return jnp.take_along_axis(before, routed, axis=1).astype(jnp.int32)

def pack_rows(token_rows, routed, expert_count, capacity):
    token_count = token_rows.shape[0]
    slot_flat = (routed * capacity + slot_table(routed, expert_count)).astype(jnp.int32)
    owners = jnp.repeat(jnp.arange(token_count, dtype=jnp.int32), 2)
    source = jnp.full((expert_count * capacity,), token_count, jnp.int32).at[slot_flat.reshape(-1)].set(owners)
    padded = jnp.concatenate([token_rows, jnp.zeros((1, token_rows.shape[1]), token_rows.dtype)], axis=0)
    return (padded[source].reshape(expert_count, capacity, token_rows.shape[1]), slot_flat)

def mix_weights(token_rows, routed, router):
    logits = jnp.dot(token_rows, router, preferred_element_type=jnp.float32)
    picked = jnp.take_along_axis(logits, routed, axis=1)
    weight_first = jax.nn.sigmoid(picked[:, 0] - picked[:, 1])
    return (weight_first, 1.0 - weight_first)

def reference(tokens, routes, router, w_gate, w_up, w_down, adapter, upstream, bound):

    def pack_one(token_rows, routed):
        return pack_rows(token_rows, routed, EXPERTS, CAP)
    packed, slot_flats = jax.vmap(pack_one)(tokens, routes)

    def add_block(running, operand_pair):
        down_piece = jnp.dot(operand_pair[0], operand_pair[1], preferred_element_type=jnp.float32).astype(jnp.bfloat16)
        down_piece = lax.optimization_barrier(down_piece)
        return (running + down_piece.astype(jnp.float32), None)

    def expert_one(inputs):
        expert_rows, gate_w, up_w, down_w = inputs
        flat_rows = expert_rows.reshape(-1, D)
        gate_out = jnp.dot(flat_rows, gate_w, preferred_element_type=jnp.float32)
        up_out = jnp.dot(flat_rows, up_w, preferred_element_type=jnp.float32)
        hidden = (jax.nn.silu(gate_out) * up_out).astype(jnp.bfloat16)
        blocks = jnp.transpose(hidden.reshape(-1, N_FFN, FF_DEV), (1, 0, 2))
        down_blocks = down_w.reshape(N_FFN, FF_DEV, D)
        running, _ = lax.scan(add_block, jnp.zeros((CLIENTS * CAP, D), jnp.float32), (blocks, down_blocks))
        return running.reshape(CLIENTS, CAP, D)
    expert_out = lax.map(expert_one, (jnp.moveaxis(packed, 1, 0), w_gate, w_up, w_down))
    by_client = jnp.moveaxis(expert_out, 0, 1).reshape(CLIENTS, EXPERTS * CAP, D)

    def client_one(inputs):
        token_rows, routed, slot_flat, expert_rows, adapt_matrix, grad_input, clip_limit = inputs
        weight_first, weight_second = mix_weights(token_rows, routed, router)
        picked = expert_rows[slot_flat]
        mixture = weight_first[:, None] * picked[:, 0] + weight_second[:, None] * picked[:, 1]
        layer_out = (token_rows.astype(jnp.float32) + mixture).astype(jnp.bfloat16)
        adapted = (layer_out.astype(jnp.float32) + jnp.dot(layer_out, adapt_matrix, preferred_element_type=jnp.float32)).astype(jnp.bfloat16)
        adapter_grad = lax.dot_general(layer_out, grad_input, (((0,), (0,)), ((), ())), preferred_element_type=jnp.float32)
        grad_norm = jnp.sqrt(jnp.sum(adapter_grad * adapter_grad))
        factor = clip_limit / jnp.maximum(grad_norm, clip_limit)
        return (adapted, (adapter_grad * factor).astype(jnp.bfloat16))
    adapted, clipped = lax.map(client_one, (tokens, routes, slot_flats, by_client, adapter, upstream, bound))
    return (adapted, clipped)
```

```python
import jax
import jax.numpy as jnp
from jax import lax
from jax.experimental import pallas as pl
from jax.experimental.pallas import tpu as pltpu
from jax.sharding import Mesh
from jax.sharding import PartitionSpec as P

FFN = ("ffn_0", "ffn_1")
BF = jnp.bfloat16
F32 = jnp.float32
I32 = jnp.int32
CAP = 48
N_EXP = 8
GRAM_ROWS = 16


VM = pl.BlockSpec(memory_space=pltpu.VMEM)
SM = pl.BlockSpec(memory_space=pltpu.SMEM)
ANY = pl.BlockSpec(memory_space=pl.ANY)


def dot(a, b, dims=(((1,), (0,)), ((), ()))):
    return lax.dot_general(a, b, dims, preferred_element_type=F32)


def params(mib=40):
    return pltpu.CompilerParams(vmem_limit_bytes=mib * 1024 * 1024)


def offset_perm(k):
    return [(x * 2 + c, ((x + k // 2) % 4) * 2 + (c ^ (k % 2))) for x in range(4) for c in range(2)]


def back_perm(k):
    return [(b, a) for a, b in offset_perm(k)]


def offset_of(route, me):
    x = me >> 1
    c = me & 1
    return ((((route >> 1) - x) & 3) << 1) + ((route & 1) ^ c)


def slot_rows(routes_t, me):
    n = routes_t.shape[1]
    r0 = routes_t[0:1, :]
    r1 = routes_t[1:2, :]
    e = lax.broadcasted_iota(I32, (N_EXP, n), 0)
    h0 = e == r0
    h1 = e == r1
    hits = (h0 | h1).astype(F32).astype(BF)
    tri = (lax.broadcasted_iota(I32, (n, n), 0) < lax.broadcasted_iota(I32, (n, n), 1)).astype(F32).astype(BF)
    before = dot(hits, tri)
    s0 = jnp.sum(jnp.where(h0, before, 0.0), axis=0, keepdims=True).astype(I32)
    s1 = jnp.sum(jnp.where(h1, before, 0.0), axis=0, keepdims=True).astype(I32)
    return offset_of(r0, me) * CAP + s0, offset_of(r1, me) * CAP + s1


def slot_cols(routes, me):
    n = routes.shape[0]
    r0 = routes[:, 0:1]
    r1 = routes[:, 1:2]
    e = lax.broadcasted_iota(I32, (n, N_EXP), 1)
    h0 = e == r0
    h1 = e == r1
    hits = (h0 | h1).astype(F32).astype(BF)
    tri = (lax.broadcasted_iota(I32, (n, n), 1) < lax.broadcasted_iota(I32, (n, n), 0)).astype(F32).astype(BF)
    before = dot(tri, hits)
    s0 = jnp.sum(jnp.where(h0, before, 0.0), axis=1, keepdims=True).astype(I32)
    s1 = jnp.sum(jnp.where(h1, before, 0.0), axis=1, keepdims=True).astype(I32)
    return offset_of(r0, me) * CAP + s0, offset_of(r1, me) * CAP + s1


def pack_body(me_ref, tok_ref, routes_ref, *outs):
    n = tok_ref.shape[0]
    row0, row1 = slot_rows(routes_ref[...], me_ref[0])
    r = lax.broadcasted_iota(I32, (N_EXP * CAP, n), 0)
    sel = ((r == row0) | (r == row1)).astype(F32).astype(BF)
    width = tok_ref.shape[1]
    step = 1024
    for j in range(0, width, step):
        got = dot(sel, tok_ref[:, j : j + step]).astype(BF)
        for k in range(N_EXP):
            outs[k][:, j : j + step] = got[k * CAP : (k + 1) * CAP]


def pack(me, tok, routes_t):
    out = jax.ShapeDtypeStruct((CAP, tok.shape[1]), BF)
    return pl.pallas_call(
        pack_body,
        out_shape=[out] * N_EXP,
        in_specs=[SM, VM, VM],
        out_specs=[VM] * N_EXP,
        compiler_params=params(),
        name="pack",
    )(me, tok, routes_t)


def expert_body(*refs):
    parts = refs[:N_EXP]
    wg, wu, wd = refs[N_EXP : N_EXP + 3]
    outs = refs[N_EXP + 3 : 2 * N_EXP + 3]
    x, vg, vu, vd, acc_g, acc_u, sem = refs[2 * N_EXP + 3 :]
    rows, width = x.shape
    copies_x = [
        pltpu.make_async_copy(parts[k], x.at[pl.ds(k * CAP, CAP)], sem.at[k]) for k in range(N_EXP)
    ]
    for c in copies_x:
        c.start()
    n_k = 4
    kb = width // n_k
    copies_w = []
    for i in range(n_k):
        s = pl.ds(i * kb, kb)
        a = pltpu.make_async_copy(wg.at[s], vg.at[s], sem.at[N_EXP + 2 * i])
        b = pltpu.make_async_copy(wu.at[s], vu.at[s], sem.at[N_EXP + 2 * i + 1])
        a.start()
        b.start()
        copies_w.append((a, b))
    cd = pltpu.make_async_copy(wd, vd, sem.at[N_EXP + 2 * n_k])
    cd.start()
    for c in copies_x:
        c.wait()
    for i in range(n_k):
        copies_w[i][0].wait()
        copies_w[i][1].wait()
        s = slice(i * kb, (i + 1) * kb)
        g = dot(x[:, s], vg[s, :])
        u = dot(x[:, s], vu[s, :])
        if i == 0:
            acc_g[...] = g
            acc_u[...] = u
        else:
            acc_g[...] += g
            acc_u[...] += u
    g = acc_g[...]
    hidden = (g / (1.0 + jnp.exp(-g)) * acc_u[...]).astype(BF)
    cd.wait()
    step = 1024
    for j in range(0, width, step):
        y = dot(hidden, vd[:, j : j + step]).astype(BF)
        for k in range(N_EXP):
            outs[k][:, j : j + step] = y[k * CAP : (k + 1) * CAP]


def experts(parts, wg, wu, wd):
    width, units = wg.shape
    rows = N_EXP * CAP
    out = jax.ShapeDtypeStruct((CAP, width), BF)
    return pl.pallas_call(
        expert_body,
        out_shape=[out] * N_EXP,
        in_specs=[ANY] * (N_EXP + 3),
        out_specs=[VM] * N_EXP,
        scratch_shapes=[
            pltpu.VMEM((rows, width), BF),
            pltpu.VMEM((width, units), BF),
            pltpu.VMEM((width, units), BF),
            pltpu.VMEM((units, width), BF),
            pltpu.VMEM((rows, units), F32),
            pltpu.VMEM((rows, units), F32),
            pltpu.SemaphoreType.DMA((N_EXP + 9,)),
        ],
        compiler_params=params(),
        name="experts",
    )(*parts, wg, wu, wd)


def three(v):
    hi = v.astype(BF)
    rest = v - hi.astype(F32)
    mid = rest.astype(BF)
    low = (rest - mid.astype(F32)).astype(BF)
    return hi, mid, low


def combine_body(me_ref, *refs):
    parts = refs[:N_EXP]
    routes_ref, mix_ref, up_ref, out, y, sem = refs[N_EXP:]
    copies = [pltpu.make_async_copy(parts[k], y.at[pl.ds(k * CAP, CAP)], sem.at[k]) for k in range(N_EXP)]
    for c in copies:
        c.start()
    n = routes_ref.shape[0]
    row0, row1 = slot_cols(routes_ref[...], me_ref[0])
    r = lax.broadcasted_iota(I32, (n, N_EXP * CAP), 1)
    p0 = (r == row0).astype(F32).astype(BF)
    p1 = (r == row1).astype(F32).astype(BF)
    w0 = mix_ref[...]
    w1 = 1.0 - w0
    up = up_ref[...]
    gram = three(dot(up, up, (((1,), (1,)), ((), ()))))
    blocks = out.shape[0]
    per = n // blocks
    zero = jnp.zeros((GRAM_ROWS - 3 * per, out.shape[2]), BF)
    for b in range(blocks):
        s = slice(b * per, (b + 1) * per)
        out[b, n : n + GRAM_ROWS, :] = jnp.concatenate([g[s].astype(F32) for g in gram] + [zero.astype(F32)], axis=0).astype(BF)
    for c in copies:
        c.wait()
    cols = out.shape[2]
    step = 4
    for b in range(0, blocks, step):
        yb = y[:, b * cols : (b + step) * cols]
        m = (w0 * dot(p0, yb) + w1 * dot(p1, yb)).astype(BF)
        for i in range(step):
            out[b + i, 0:n, :] = m[:, i * cols : (i + 1) * cols]


def combine(me, parts, routes, mix, up, blocks):
    n = routes.shape[0]
    width = parts[0].shape[1]
    return pl.pallas_call(
        combine_body,
        out_shape=jax.ShapeDtypeStruct((blocks, n + GRAM_ROWS, width // blocks), BF),
        in_specs=[SM] + [ANY] * N_EXP + [VM] * 3,
        out_specs=VM,
        scratch_shapes=[pltpu.VMEM((N_EXP * CAP, width), BF), pltpu.SemaphoreType.DMA((N_EXP,))],
        compiler_params=params(),
        name="combine",
    )(me, *parts, routes, mix, up)


def layer_body(got_ref, tok_ref, out):
    blocks, rows, cols = got_ref.shape
    n = tok_ref.shape[0]
    per = n // blocks
    total = got_ref[0].astype(F32)
    for b in range(1, blocks):
        total = total + got_ref[b].astype(F32)
    out[0:n, :] = (tok_ref[...].astype(F32) + total[0:n]).astype(BF)
    g = total[n : n + per] + total[n + per : n + 2 * per] + total[n + 2 * per : n + 3 * per]
    parts = three(g)
    zero = jnp.zeros((GRAM_ROWS - 3 * per, cols), F32)
    out[n : n + GRAM_ROWS, :] = jnp.concatenate([p.astype(F32) for p in parts] + [zero], axis=0).astype(BF)


def layer_sum(got, tok_cols):
    return pl.pallas_call(
        layer_body,
        out_shape=jax.ShapeDtypeStruct(got.shape[1:], BF),
        in_specs=[VM, VM],
        out_specs=VM,
        compiler_params=params(),
        name="layer_sum",
    )(got, tok_cols)


def final_body(bound_ref, all_ref, own_ref, adapter_ref, up_ref, adapted, clipped, grad, gram):
    blocks, rows, cols = all_ref.shape
    n = up_ref.shape[0]
    per = n // blocks
    up = up_ref[...]
    acc = own_ref[0:n, :].astype(F32)
    gl = jnp.zeros((n, n), F32)
    for b in range(blocks):
        block = all_ref[b, 0:n, :]
        acc = acc + dot(block, adapter_ref[b * cols : (b + 1) * cols, :])
        gl = gl + dot(block, block, (((1,), (1,)), ((), ())))
        grad[b * cols : (b + 1) * cols, :] = dot(block, up, (((0,), (0,)), ((), ())))
        extra = all_ref[b, n : n + GRAM_ROWS, :].astype(F32)
        gram[b * per : (b + 1) * per, :] = extra[0:per] + extra[per : 2 * per] + extra[2 * per : 3 * per]
    adapted[...] = acc.astype(BF)
    norm = jnp.sqrt(jnp.maximum(jnp.sum(gl * gram[...], keepdims=True), 0.0))
    limit = bound_ref[0]
    factor = limit / jnp.maximum(norm, limit)
    for b in range(blocks):
        s = slice(b * cols, (b + 1) * cols)
        clipped[s, :] = (grad[s, :] * factor).astype(BF)


def final(bound, everything, own, adapter, up):
    n, cols = up.shape
    width = adapter.shape[0]
    return pl.pallas_call(
        final_body,
        out_shape=[jax.ShapeDtypeStruct((n, cols), BF), jax.ShapeDtypeStruct((width, cols), BF)],
        in_specs=[SM, VM, VM, VM, VM],
        out_specs=[VM, VM],
        scratch_shapes=[pltpu.VMEM((width, cols), F32), pltpu.VMEM((n, n), F32)],
        compiler_params=params(),
        name="final",
    )(bound, everything, own, adapter, up)


def spread(value, axis):
    copies = jnp.broadcast_to(value, (lax.axis_size(axis), *value.shape))
    return lax.all_to_all(copies, axis, split_axis=0, concat_axis=0, tiled=True)


def per_device(tokens, routes, router, w_gate, w_up, w_down, adapter, upstream, bound):
    me = lax.axis_index("expert").astype(I32)[None]
    blocks = lax.axis_size(FFN)
    routed = routes[0]
    tok = spread(tokens[0], FFN).reshape(-1, tokens.shape[2])
    cols = adapter.shape[2]
    outgoing = pack(me, tok, routed.T)
    arrived = [outgoing[0]] + [
        lax.ppermute(outgoing[k], "expert", offset_perm(k)) for k in range(1, N_EXP)
    ]
    logits = jnp.dot(tok, router, preferred_element_type=F32)
    chosen = routed[:, :, None] == jnp.arange(N_EXP, dtype=I32)
    picked = jnp.sum(jnp.where(chosen, logits[:, None, :], 0.0), axis=2)
    mix = jax.nn.sigmoid(picked[:, 0:1] - picked[:, 1:2])
    own_tok = lax.dynamic_slice_in_dim(tok, lax.axis_index(FFN) * cols, cols, 1)
    pieces = experts(arrived, w_gate[0], w_up[0], w_down[0])
    returned = [pieces[0]] + [
        lax.ppermute(pieces[k], "expert", back_perm(k)) for k in range(1, N_EXP)
    ]
    sums = combine(me, returned, routed, mix, upstream[0], blocks)
    got = lax.all_to_all(sums, FFN, split_axis=0, concat_axis=0, tiled=True)
    own = layer_sum(got, own_tok)
    everything = spread(own, FFN)
    adapted, clipped = final(bound, everything, own, adapter[0], upstream[0])
    return (adapted[None], clipped[None])


def solution(mesh):
    split = Mesh(mesh.devices.reshape(mesh.shape["expert"], 8, 4), ("expert", "ffn_0", "ffn_1"))
    placed = (
        P("expert", FFN, None),
        P("expert", None, None),
        P(),
        P("expert", None, FFN),
        P("expert", None, FFN),
        P("expert", FFN, None),
        P("expert", None, FFN),
        P("expert", None, FFN),
        P("expert"),
    )
    return jax.shard_map(
        per_device,
        mesh=split,
        in_specs=placed,
        out_specs=(P("expert", None, FFN), P("expert", None, FFN)),
        check_vma=False,
    )
```

```python
import jax
import jax.numpy as jnp
from jax import lax
from jax.experimental import pallas as pl
from jax.experimental.pallas import tpu as pltpu
from jax.sharding import Mesh
from jax.sharding import PartitionSpec as P

FFN = ("ffn_0", "ffn_1")
BF = jnp.bfloat16
F32 = jnp.float32
I32 = jnp.int32
CAP = 48
N_EXP = 8


VM = pl.BlockSpec(memory_space=pltpu.VMEM)
SM = pl.BlockSpec(memory_space=pltpu.SMEM)
ANY = pl.BlockSpec(memory_space=pl.ANY)
HB = pl.BlockSpec(memory_space=pltpu.HBM)


def dot(a, b, dims=(((1,), (0,)), ((), ()))):
    return lax.dot_general(a, b, dims, preferred_element_type=F32)


def params(mib=40):
    return pltpu.CompilerParams(vmem_limit_bytes=mib * 1024 * 1024)

Z = "ffn_0"
Y = "ffn_1"
N_Q = 4
HALF = N_EXP * CAP // 2
LOGIT_ROWS = 16
LANES = 128


def ring(n, k):
    return [(i, (i + k) % n) for i in range(n)]


def hop(value, k):
    return lax.ppermute(value, Y, ring(N_Q, k))


def two(v):
    hi = v.astype(BF)
    return hi, (v - hi.astype(F32)).astype(BF)


def three(v):
    hi = v.astype(BF)
    return (hi, *two(v - hi.astype(F32)))


def quarter(ids, shift):
    return (ids[2] + shift) & (N_Q - 1)


def hits_of(routes_t):
    n = routes_t.shape[1]
    e = lax.broadcasted_iota(I32, (N_EXP, n), 0)
    return e == routes_t[0:1, :], e == routes_t[1:2, :]


def slot_rows(routes_t):
    n = routes_t.shape[1]
    h0, h1 = hits_of(routes_t)
    hits = (h0 | h1).astype(F32).astype(BF)
    tri = (lax.broadcasted_iota(I32, (n, n), 0) < lax.broadcasted_iota(I32, (n, n), 1)).astype(F32).astype(BF)
    before = dot(hits, tri)
    s0 = jnp.sum(jnp.where(h0, before, 0.0), axis=0, keepdims=True).astype(I32)
    s1 = jnp.sum(jnp.where(h1, before, 0.0), axis=0, keepdims=True).astype(I32)
    return routes_t[0:1, :] * CAP + s0, routes_t[1:2, :] * CAP + s1


def column(row):
    n = row.shape[1]
    diag = lax.broadcasted_iota(I32, (n, n), 0) == lax.broadcasted_iota(I32, (n, n), 1)
    return jnp.sum(jnp.where(diag, jnp.broadcast_to(row, (n, n)), 0.0), axis=1, keepdims=True)


def pack_body(tok_ref, routes_ref, out):
    n = tok_ref.shape[0]
    row0, row1 = slot_rows(routes_ref[...])
    r = lax.broadcasted_iota(I32, (N_EXP * CAP, n), 0)
    sel = ((r == row0) | (r == row1)).astype(F32).astype(BF)
    out[...] = dot(sel, tok_ref[...]).astype(BF)


def pack(tok, routes_t):
    return pl.pallas_call(
        pack_body,
        out_shape=jax.ShapeDtypeStruct((N_EXP * CAP, tok.shape[1]), BF),
        in_specs=[VM, VM],
        out_specs=VM,
        compiler_params=params(),
        name="pack",
    )(tok, routes_t)


def halve_body(ids, x_ref, tok_ref, router_ref, out0, out1):
    width = tok_ref.shape[1]
    start = pl.multiple_of(ids[2] * width, LANES)
    logits = dot(router_ref[:, pl.ds(start, width)], tok_ref[...], (((1,), (1,)), ((), ())))
    n = logits.shape[1]
    parts = three(logits)
    wide = jnp.concatenate([p.astype(F32) for p in parts] + [jnp.zeros((N_EXP, width - 3 * n), F32)], axis=1)
    wide = jnp.concatenate([wide, jnp.zeros((LOGIT_ROWS - N_EXP, width), F32)], axis=0)
    out0[0:HALF, :] = x_ref[0:HALF, :]
    out0[HALF : HALF + LOGIT_ROWS, :] = wide.astype(BF)
    out1[...] = x_ref[HALF:, :]


def halve(ids, x, tok, router_t):
    width = x.shape[1]
    return pl.pallas_call(
        halve_body,
        out_shape=[
            jax.ShapeDtypeStruct((HALF + LOGIT_ROWS, width), BF),
            jax.ShapeDtypeStruct((HALF, width), BF),
        ],
        in_specs=[SM, VM, VM, VM],
        out_specs=[VM, VM],
        compiler_params=params(),
        name="halve",
    )(ids, x, tok, router_t)


def gate_steps(ids, shifts, halves, wg, wu, x, vg, vu, sem):
    width = x.shape[2]
    started = []
    for i, shift in enumerate(shifts):
        rows = pl.ds(pl.multiple_of(quarter(ids, shift) * width, LANES), width)
        h0, h1 = halves[2 * i], halves[2 * i + 1]
        copies = [
            pltpu.make_async_copy(h0.at[pl.ds(0, HALF)], x.at[i, pl.ds(0, HALF)], sem.at[4 * i]),
            pltpu.make_async_copy(h1, x.at[i, pl.ds(HALF, HALF)], sem.at[4 * i + 1]),
            pltpu.make_async_copy(wg.at[rows], vg.at[i], sem.at[4 * i + 2]),
            pltpu.make_async_copy(wu.at[rows], vu.at[i], sem.at[4 * i + 3]),
        ]
        for c in copies:
            c.start()
        started.append(copies)

    def finish(i):
        for c in started[i]:
            c.wait()
        return dot(x[i], vg[i]), dot(x[i], vu[i])

    return finish


def gates_body(shifts, first, ids, *refs):
    n = 2 * len(shifts)
    halves = refs[:n]
    wg, wu = refs[n : n + 2]
    rest = refs[n + 2 :]
    if first:
        out_g, out_u, x, vg, vu, sem = rest
    else:
        in_g, in_u, out_g, out_u, x, vg, vu, sem = rest
    finish = gate_steps(ids, shifts, halves, wg, wu, x, vg, vu, sem)
    for i in range(len(shifts)):
        g, u = finish(i)
        if i == 0 and first:
            out_g[...] = g
            out_u[...] = u
        elif i == 0:
            out_g[...] = in_g[...] + g
            out_u[...] = in_u[...] + u
        else:
            out_g[...] += g
            out_u[...] += u


def gate_scratch(n, width, units):
    rows = N_EXP * CAP
    return [
        pltpu.VMEM((n, rows, width), BF),
        pltpu.VMEM((n, width, units), BF),
        pltpu.VMEM((n, width, units), BF),
        pltpu.SemaphoreType.DMA((4 * n,)),
    ]


def flops(n, width, units):
    work = 4 * n * N_EXP * CAP * width * units
    return pl.CostEstimate(flops=work, bytes_accessed=4 * n * width * units, transcendentals=0)


def gates(ids, shifts, halves, wg, wu, acc=()):
    n = len(shifts)
    width = halves[0].shape[1]
    units = wg.shape[1]
    out = jax.ShapeDtypeStruct((N_EXP * CAP, units), F32)

    def body(*refs):
        gates_body(shifts, not acc, *refs)

    return pl.pallas_call(
        body,
        out_shape=[out, out],
        in_specs=[SM] + [ANY] * (2 * n) + [HB, HB] + [VM] * len(acc),
        out_specs=[VM, VM],
        scratch_shapes=gate_scratch(n, width, units),
        compiler_params=params(),
        cost_estimate=flops(n, width, units),
        name=f"gates{n}",
    )(ids, *halves, wg, wu, *acc)


def turn_body(ids, h0, h1, wg, wu, wd, in_g, in_u, hidden_ref, out0, out1, x, vg, vu, sem, vd, sem_d):
    width = x.shape[2]
    cols = pl.ds(pl.multiple_of(quarter(ids, 2) * width, LANES), width)
    finish = gate_steps(ids, (2,), (h0, h1), wg, wu, x, vg, vu, sem)
    down = pltpu.make_async_copy(wd.at[:, cols], vd, sem_d.at[0])
    down.start()
    g, u = finish(0)
    g = in_g[...] + g
    u = in_u[...] + u
    hidden = (g / (1.0 + jnp.exp(-g)) * u).astype(BF)
    hidden_ref[...] = hidden
    down.wait()
    y = dot(hidden, vd[...]).astype(BF)
    out0[...] = y[:HALF]
    out1[...] = y[HALF:]


def turn(ids, h0, h1, wg, wu, wd, acc):
    width = h1.shape[1]
    units = wg.shape[1]
    half = jax.ShapeDtypeStruct((HALF, width), BF)
    return pl.pallas_call(
        turn_body,
        out_shape=[jax.ShapeDtypeStruct((N_EXP * CAP, units), BF), half, half],
        in_specs=[SM, ANY, ANY, HB, HB, HB, VM, VM],
        out_specs=[VM, VM, VM],
        scratch_shapes=gate_scratch(1, width, units)
        + [pltpu.VMEM((units, width), BF), pltpu.SemaphoreType.DMA((1,))],
        compiler_params=params(),
        cost_estimate=flops(1, width, units),
        name="turn",
    )(ids, h0, h1, wg, wu, wd, *acc)


def downs_body(ids, hidden_ref, wd, *refs):
    outs = refs[:6]
    vd, sem = refs[6:]
    width = vd.shape[2]
    copies = []
    for i, shift in enumerate((1, 3, 0)):
        cols = pl.ds(pl.multiple_of(quarter(ids, shift) * width, LANES), width)
        copies.append(pltpu.make_async_copy(wd.at[:, cols], vd.at[i], sem.at[i]))
        copies[-1].start()
    for i in range(3):
        copies[i].wait()
        y = dot(hidden_ref[...], vd[i]).astype(BF)
        outs[2 * i][...] = y[:HALF]
        outs[2 * i + 1][...] = y[HALF:]


def downs(ids, hidden, wd):
    units, full = wd.shape
    width = full // N_Q
    half = jax.ShapeDtypeStruct((HALF, width), BF)
    return pl.pallas_call(
        downs_body,
        out_shape=[half] * 6,
        in_specs=[SM, VM, HB],
        out_specs=[VM] * 6,
        scratch_shapes=[pltpu.VMEM((3, units, width), BF), pltpu.SemaphoreType.DMA((3,))],
        compiler_params=params(),
        cost_estimate=flops(1, width, units),
        name="downs",
    )(ids, hidden, wd)


def add_body(a0, b0, a1, b1, out0, out1):
    out0[...] = (a0[...].astype(F32) + b0[...].astype(F32)).astype(BF)
    out1[...] = (a1[...].astype(F32) + b1[...].astype(F32)).astype(BF)


def add_pairs(a0, b0, a1, b1):
    half = jax.ShapeDtypeStruct(a0.shape, BF)
    return pl.pallas_call(
        add_body,
        out_shape=[half, half],
        in_specs=[VM] * 4,
        out_specs=[VM] * 2,
        compiler_params=params(),
        name="add_pairs",
    )(a0, b0, a1, b1)


def gather_sum_body(o0, a0, b0, o1, a1, b1, out):
    out[0:HALF, :] = (o0[...].astype(F32) + a0[...].astype(F32) + b0[...].astype(F32)).astype(BF)
    out[HALF:, :] = (o1[...].astype(F32) + a1[...].astype(F32) + b1[...].astype(F32)).astype(BF)


def gather_sum(*args):
    width = args[0].shape[1]
    return pl.pallas_call(
        gather_sum_body,
        out_shape=jax.ShapeDtypeStruct((2 * HALF, width), BF),
        in_specs=[VM] * 6,
        out_specs=VM,
        compiler_params=params(),
        name="gather_sum",
    )(*args)


def combine_body(y_ref, routes_ref, l0, l1, l2, l3, up_ref, out, lv, sem):
    copies = []
    for i, l in enumerate((l0, l1, l2, l3)):
        copies.append(pltpu.make_async_copy(l.at[pl.ds(HALF, LOGIT_ROWS)], lv.at[i], sem.at[i]))
        copies[-1].start()
    blocks, _, cols = out.shape
    up = up_ref[...]
    n = up.shape[0]
    per = n // blocks
    gram = [p.astype(F32) for p in two(dot(up, up, (((1,), (1,)), ((), ()))))]
    for b in range(blocks):
        s = slice(b * per, (b + 1) * per)
        out[b, n : n + 2 * per, :] = jnp.concatenate([g[s] for g in gram], axis=0).astype(BF)
    routes_t = routes_ref[...]
    h0, h1 = hits_of(routes_t)
    row0, row1 = slot_rows(routes_t)
    r = lax.broadcasted_iota(I32, (N_EXP * CAP, n), 0)
    p0 = (r == row0).astype(F32).T.astype(BF)
    p1 = (r == row1).astype(F32).T.astype(BF)
    for c in copies:
        c.wait()
    logits = jnp.zeros((N_EXP, n), F32)
    for i in range(N_Q):
        rows = lv[i].astype(F32)
        logits = logits + (rows[0:N_EXP, 0:n] + rows[0:N_EXP, n : 2 * n] + rows[0:N_EXP, 2 * n : 3 * n])
    picked0 = jnp.sum(jnp.where(h0, logits, 0.0), axis=0, keepdims=True)
    picked1 = jnp.sum(jnp.where(h1, logits, 0.0), axis=0, keepdims=True)
    w0 = column(1.0 / (1.0 + jnp.exp(picked1 - picked0)))
    w1 = 1.0 - w0
    y = y_ref[...]
    mix = (w0 * dot(p0, y) + w1 * dot(p1, y)).astype(BF)
    for b in range(blocks):
        out[b, 0:n, :] = mix[:, b * cols : (b + 1) * cols]


def combine(y, routes_t, logits, up, blocks):
    n = routes_t.shape[1]
    width = y.shape[1]
    return pl.pallas_call(
        combine_body,
        out_shape=jax.ShapeDtypeStruct((blocks, n + 2 * (n // blocks), width // blocks), BF),
        in_specs=[VM, VM] + [ANY] * 4 + [VM],
        out_specs=VM,
        scratch_shapes=[pltpu.VMEM((4, LOGIT_ROWS, width), BF), pltpu.SemaphoreType.DMA((4,))],
        compiler_params=params(),
        name="combine",
    )(y, routes_t, *logits, up)


def layer_body(ids, got_ref, tok_ref, out):
    blocks, rows, cols = got_ref.shape
    n = tok_ref.shape[0]
    per = n // blocks
    total = got_ref[0].astype(F32)
    for b in range(1, blocks):
        total = total + got_ref[b].astype(F32)
    tok = tok_ref[:, pl.ds(pl.multiple_of(ids[1] * cols, LANES), cols)]
    layer = (tok.astype(F32) + total[0:n]).astype(BF)
    parts = two(total[n : n + per] + total[n + per : n + 2 * per])
    extra = jnp.concatenate([p.astype(F32) for p in parts], axis=0).astype(BF)
    for b in range(blocks):
        out[b, 0:n, :] = layer
        out[b, n : n + 2 * per, :] = extra


def layer_sum(ids, got, tok):
    return pl.pallas_call(
        layer_body,
        out_shape=jax.ShapeDtypeStruct(got.shape, BF),
        in_specs=[SM, VM, VM],
        out_specs=VM,
        compiler_params=params(),
        name="layer_sum",
    )(ids, got, tok)


def final_body(ids, bound_ref, q0, q1, q2, q3, adapter_ref, up_ref, adapted, clipped, grad, gram):
    blocks, rows, cols = q0.shape
    n = up_ref.shape[0]
    per = n // blocks
    up = up_ref[...]
    mine = ids[1] * N_Q + ids[2]
    acc = jnp.zeros((n, cols), F32)
    gl = jnp.zeros((n, n), F32)
    for i, (q, shift) in enumerate(((q0, 0), (q1, 3), (q2, 1), (q3, 2))):
        where = quarter(ids, shift)
        own = q[lax.rem(mine, blocks), 0:n, :].astype(F32)
        acc = acc + jnp.where(lax.div(mine, blocks) == where, own, 0.0)
        for b in range(blocks):
            s = pl.ds(pl.multiple_of((where * blocks + b) * cols, LANES), cols)
            block = q[b, 0:n, :]
            acc = acc + dot(block, adapter_ref[s, :])
            gl = gl + dot(block, block, (((1,), (1,)), ((), ())))
            grad[s, :] = dot(block, up, (((0,), (0,)), ((), ())))
            extra = q[b, n : n + 2 * per, :].astype(F32)
            piece = extra[0:per] + extra[per : 2 * per]
            if i == 0:
                gram[b * per : (b + 1) * per, :] = piece
            else:
                gram[b * per : (b + 1) * per, :] += piece
    adapted[...] = acc.astype(BF)
    norm = jnp.sqrt(jnp.maximum(jnp.sum(gl * gram[...], keepdims=True), 0.0))
    limit = bound_ref[0]
    factor = limit / jnp.maximum(norm, limit)
    for b in range(N_Q * blocks):
        s = slice(b * cols, (b + 1) * cols)
        clipped[s, :] = (grad[s, :] * factor).astype(BF)


def final(ids, bound, quarters, adapter, up):
    n, cols = up.shape
    width = adapter.shape[0]
    return pl.pallas_call(
        final_body,
        out_shape=[jax.ShapeDtypeStruct((n, cols), BF), jax.ShapeDtypeStruct((width, cols), BF)],
        in_specs=[SM, SM] + [VM] * 6,
        out_specs=[VM, VM],
        scratch_shapes=[pltpu.VMEM((width, cols), F32), pltpu.VMEM((n, n), F32)],
        compiler_params=params(),
        name="final",
    )(ids, bound, *quarters, adapter, up)


def exchange(value, axis):
    return lax.all_to_all(value, axis, split_axis=0, concat_axis=0, tiled=True)


def per_device(tokens, routes, router, w_gate, w_up, w_down, adapter, upstream, bound):
    ids = jnp.stack([lax.axis_index(a) for a in ("expert", Z, Y)]).astype(I32)
    n_z = lax.axis_size(Z)
    mine, width = tokens.shape[1:]
    q_width = width // N_Q
    routes_t = routes[0].T
    wg, wu, wd = w_gate[0], w_up[0], w_down[0]
    up = upstream[0]
    cut = jnp.transpose(tokens[0].reshape(mine, N_Q, q_width), (1, 0, 2))
    cut = jnp.broadcast_to(cut, (n_z, N_Q, mine, q_width)).reshape(n_z * N_Q, mine, q_width)
    tok = exchange(cut, FFN).reshape(-1, q_width)
    packed = pack(tok, routes_t)
    x = exchange(packed.reshape(N_EXP, CAP, q_width), "expert").reshape(N_EXP * CAP, q_width)
    h0, h1 = halve(ids, x, tok, router.T)
    a0 = hop(h0, 1)
    b1 = hop(h1, -1)
    a1 = hop(h1, 1)
    b0 = hop(h0, -1)
    acc = gates(ids, (0,), (h0, h1), wg, wu)
    c0 = hop(a0, 1)
    c1 = hop(b1, -1)
    acc = gates(ids, (3, 1), (a0, a1, b0, b1), wg, wu, acc)
    hidden, d0, d1 = turn(ids, c0, c1, wg, wu, wd, acc)
    r0 = hop(d0, 1)
    r1 = hop(d1, -1)
    p0, p1, m0, m1, o0, o1 = downs(ids, hidden, wd)
    s1 = hop(p1, 1)
    s0 = hop(m0, -1)
    p0, m1 = add_pairs(p0, r0, m1, r1)
    t0 = hop(p0, 1)
    t1 = hop(m1, -1)
    total = gather_sum(o0, s0, t0, o1, s1, t1)
    back = exchange(total.reshape(N_EXP, CAP, q_width), "expert").reshape(N_EXP * CAP, q_width)
    sums = combine(back, routes_t, (h0, a0, b0, c0), up, n_z)
    layer = layer_sum(ids, exchange(sums, Z), tok)
    layer = exchange(layer, Z)
    quarters = (layer, hop(layer, 1), hop(layer, -1), hop(layer, 2))
    adapted, clipped = final(ids, bound, quarters, adapter[0], up)
    return (adapted[None], clipped[None])


def solution(mesh):
    split = Mesh(mesh.devices.reshape(mesh.shape["expert"], 8, 4), ("expert", "ffn_0", "ffn_1"))
    placed = (
        P("expert", FFN, None),
        P("expert", None, None),
        P(),
        P("expert", None, FFN),
        P("expert", None, FFN),
        P("expert", FFN, None),
        P("expert", None, FFN),
        P("expert", None, FFN),
        P("expert"),
    )
    return jax.shard_map(
        per_device,
        mesh=split,
        in_specs=placed,
        out_specs=(P("expert", None, FFN), P("expert", None, FFN)),
        check_vma=False,
    )
```

```python
import jax
import jax.numpy as jnp
from jax import lax
from jax.experimental import pallas as pl
from jax.experimental.pallas import tpu as pltpu
from jax.sharding import Mesh
from jax.sharding import PartitionSpec as P

FFN = ("ffn_0", "ffn_1")
BF = jnp.bfloat16
F32 = jnp.float32
I32 = jnp.int32
CAP = 48
N_EXP = 8


VM = pl.BlockSpec(memory_space=pltpu.VMEM)
SM = pl.BlockSpec(memory_space=pltpu.SMEM)
ANY = pl.BlockSpec(memory_space=pl.ANY)
HB = pl.BlockSpec(memory_space=pltpu.HBM)


def dot(a, b, dims=(((1,), (0,)), ((), ()))):
    return lax.dot_general(a, b, dims, preferred_element_type=F32)


def params(mib=40):
    return pltpu.CompilerParams(vmem_limit_bytes=mib * 1024 * 1024)

Z = "ffn_0"
Y = "ffn_1"
N_Q = 4
HALF = N_EXP * CAP // 2
LANES = 128


def ring(n, k):
    return [(i, (i + k) % n) for i in range(n)]


def y_hop(value, k):
    return lax.ppermute(value, Y, ring(N_Q, k))


def z_hop(value, k):
    return lax.ppermute(value, Z, ring(lax.axis_size(Z), k))


def two(v):
    hi = v.astype(BF)
    return hi, (v - hi.astype(F32)).astype(BF)


def three(v):
    hi = v.astype(BF)
    return (hi, *two(v - hi.astype(F32)))


def quarter(ids, shift):
    return (ids[2] + 2 * (ids[1] & 1) + shift) & (N_Q - 1)


def holders(n_z):
    return [[z * N_Q + (q + 2 * (z % 2)) % N_Q for z in range(n_z)] for q in range(N_Q)]


def hits_of(routes_t):
    n = routes_t.shape[1]
    e = lax.broadcasted_iota(I32, (N_EXP, n), 0)
    return e == routes_t[0:1, :], e == routes_t[1:2, :]


def slot_rows(routes_t):
    n = routes_t.shape[1]
    h0, h1 = hits_of(routes_t)
    hits = (h0 | h1).astype(F32).astype(BF)
    tri = (lax.broadcasted_iota(I32, (n, n), 0) < lax.broadcasted_iota(I32, (n, n), 1)).astype(F32).astype(BF)
    before = dot(hits, tri)
    s0 = jnp.sum(jnp.where(h0, before, 0.0), axis=0, keepdims=True).astype(I32)
    s1 = jnp.sum(jnp.where(h1, before, 0.0), axis=0, keepdims=True).astype(I32)
    return routes_t[0:1, :] * CAP + s0, routes_t[1:2, :] * CAP + s1


def fill_body(tok_ref, router_ref, out):
    dests, mine, full = out.shape
    width = full - LANES
    tok = tok_ref[...]
    logits = dot(tok, router_ref[...], (((1,), (1,)), ((), ())))
    parts = [p.astype(F32) for p in three(logits)]
    extra = jnp.concatenate(parts + [jnp.zeros((mine, LANES - 3 * N_EXP), F32)], axis=1).astype(BF)
    for d in range(dests):
        q = (d % N_Q + 2 * (d // N_Q % 2)) % N_Q
        out[d, :, 0:width] = tok[:, q * width : (q + 1) * width]
        out[d, :, width:] = extra


def fill(tok, router_t, dests):
    mine, full = tok.shape
    return pl.pallas_call(
        fill_body,
        out_shape=jax.ShapeDtypeStruct((dests, mine, full // N_Q + LANES), BF),
        in_specs=[VM, VM],
        out_specs=VM,
        compiler_params=params(),
        name="fill",
    )(tok, router_t)


def pack_body(tok_ref, routes_ref, out):
    n = tok_ref.shape[0]
    row0, row1 = slot_rows(routes_ref[...])
    r = lax.broadcasted_iota(I32, (N_EXP * CAP, n), 0)
    sel = ((r == row0) | (r == row1)).astype(F32).astype(BF)
    out[...] = dot(sel, tok_ref[:, 0 : out.shape[1]]).astype(BF)


def pack(tok, routes_t):
    return pl.pallas_call(
        pack_body,
        out_shape=jax.ShapeDtypeStruct((N_EXP * CAP, tok.shape[1] - LANES), BF),
        in_specs=[VM, VM],
        out_specs=VM,
        compiler_params=params(),
        name="pack",
    )(tok, routes_t)


def gate_steps(ids, plan, wg, wu, x, vg, vu, sem):
    width = x.shape[2]
    started = []
    count = 0
    for i, (shift, pieces) in enumerate(plan):
        rows = pl.ds(pl.multiple_of(quarter(ids, shift) * width, LANES), width)
        pairs = [(p, x.at[i, pl.ds(r, p.shape[0])]) for p, r in pieces]
        pairs += [(wg.at[rows], vg.at[i]), (wu.at[rows], vu.at[i])]
        copies = []
        for a, b in pairs:
            copies.append(pltpu.make_async_copy(a, b, sem.at[count]))
            copies[-1].start()
            count += 1
        started.append(copies)

    def finish(i):
        for c in started[i]:
            c.wait()
        return dot(x[i], vg[i]), dot(x[i], vu[i])

    return finish


def gate_scratch(n, width, units):
    rows = N_EXP * CAP
    return [
        pltpu.VMEM((n, rows, width), BF),
        pltpu.VMEM((n, width, units), BF),
        pltpu.VMEM((n, width, units), BF),
        pltpu.SemaphoreType.DMA((4 * n,)),
    ]


def flops(n, width, units):
    work = 4 * n * N_EXP * CAP * width * units
    return pl.CostEstimate(flops=work, bytes_accessed=4 * n * width * units, transcendentals=0)


def own_body(ids, x_ref, wg, wu, out_g, out_u, x, vg, vu, sem):
    finish = gate_steps(ids, [(0, [(x_ref, 0)])], wg, wu, x, vg, vu, sem)
    out_g[...], out_u[...] = finish(0)


def far_body(ids, c0, c1, wg, wu, in_g, in_u, out_g, out_u, x, vg, vu, sem):
    finish = gate_steps(ids, [(2, [(c0, 0), (c1, HALF)])], wg, wu, x, vg, vu, sem)
    g, u = finish(0)
    out_g[...] = in_g[...] + g
    out_u[...] = in_u[...] + u


def gates(body, ids, pieces, wg, wu, acc=()):
    width = pieces[0].shape[1]
    units = wg.shape[1]
    out = jax.ShapeDtypeStruct((N_EXP * CAP, units), F32)
    return pl.pallas_call(
        body,
        out_shape=[out, out],
        in_specs=[SM] + [ANY] * len(pieces) + [HB, HB] + [VM] * len(acc),
        out_specs=[VM, VM],
        scratch_shapes=gate_scratch(1, width, units),
        compiler_params=params(),
        cost_estimate=flops(1, width, units),
        name="gates",
    )(ids, *pieces, wg, wu, *acc)


def start_downs(ids, shifts, wd, vd, sem):
    width = vd.shape[2]
    copies = []
    for i, shift in enumerate(shifts):
        cols = pl.ds(pl.multiple_of(quarter(ids, shift) * width, LANES), width)
        copies.append(pltpu.make_async_copy(wd.at[:, cols], vd.at[i], sem.at[i]))
        copies[-1].start()
    return copies


def turn_body(ids, a, b, wg, wu, wd, in_g, in_u, hidden_ref, out0, out1, x, vg, vu, sem, vd, sem_d):
    finish = gate_steps(ids, [(3, [(a, 0)]), (1, [(b, 0)])], wg, wu, x, vg, vu, sem)
    copies = start_downs(ids, (1, 3), wd, vd, sem_d)
    g0, u0 = finish(0)
    g1, u1 = finish(1)
    g = in_g[...] + g0 + g1
    u = in_u[...] + u0 + u1
    hidden = (g / (1.0 + jnp.exp(-g)) * u).astype(BF)
    hidden_ref[...] = hidden
    for i, out in enumerate((out0, out1)):
        copies[i].wait()
        out[...] = dot(hidden, vd[i]).astype(BF)


def turn(ids, a, b, wg, wu, wd, acc):
    rows, width = a.shape
    units = wg.shape[1]
    out = jax.ShapeDtypeStruct((rows, width), BF)
    return pl.pallas_call(
        turn_body,
        out_shape=[jax.ShapeDtypeStruct((rows, units), BF), out, out],
        in_specs=[SM, ANY, ANY, HB, HB, HB, VM, VM],
        out_specs=[VM, VM, VM],
        scratch_shapes=gate_scratch(2, width, units)
        + [pltpu.VMEM((2, units, width), BF), pltpu.SemaphoreType.DMA((2,))],
        compiler_params=params(),
        cost_estimate=flops(3, width, units),
        name="turn",
    )(ids, a, b, wg, wu, wd, *acc)


def downs_body(ids, hidden_ref, wd, out0, out1, own, vd, sem):
    copies = start_downs(ids, (2, 0), wd, vd, sem)
    copies[0].wait()
    y = dot(hidden_ref[...], vd[0]).astype(BF)
    out0[...] = y[:HALF]
    out1[...] = y[HALF:]
    copies[1].wait()
    own[...] = dot(hidden_ref[...], vd[1]).astype(BF)


def downs(ids, hidden, wd):
    units, full = wd.shape
    width = full // N_Q
    half = jax.ShapeDtypeStruct((HALF, width), BF)
    return pl.pallas_call(
        downs_body,
        out_shape=[half, half, jax.ShapeDtypeStruct((2 * HALF, width), BF)],
        in_specs=[SM, VM, HB],
        out_specs=[VM] * 3,
        scratch_shapes=[pltpu.VMEM((2, units, width), BF), pltpu.SemaphoreType.DMA((2,))],
        compiler_params=params(),
        cost_estimate=flops(1, width, units),
        name="downs",
    )(ids, hidden, wd)


def gather_sum_body(o, a, b, c0, c1, out):
    for s, c in ((slice(0, HALF), c0), (slice(HALF, 2 * HALF), c1)):
        out[s, :] = (o[s, :].astype(F32) + a[s, :].astype(F32) + b[s, :].astype(F32) + c[...].astype(F32)).astype(BF)


def gather_sum(*args):
    return pl.pallas_call(
        gather_sum_body,
        out_shape=jax.ShapeDtypeStruct(args[0].shape, BF),
        in_specs=[VM] * 5,
        out_specs=VM,
        compiler_params=params(),
        name="gather_sum",
    )(*args)


def combine_body(y_ref, routes_ref, routes_t_ref, tok_ref, up_ref, out):
    blocks, _, cols = out.shape
    up = up_ref[...]
    n = up.shape[0]
    per = n // blocks
    gram = [p.astype(F32) for p in two(dot(up, up, (((1,), (1,)), ((), ()))))]
    for b in range(blocks):
        s = slice(b * per, (b + 1) * per)
        out[b, n : n + 2 * per, :] = jnp.concatenate([g[s] for g in gram], axis=0).astype(BF)
    row0, row1 = slot_rows(routes_t_ref[...])
    r = lax.broadcasted_iota(I32, (N_EXP * CAP, n), 0)
    p0 = (r == row0).astype(F32).T.astype(BF)
    p1 = (r == row1).astype(F32).T.astype(BF)
    extra = tok_ref[:, y_ref.shape[1] :].astype(F32)
    logits = extra[:, 0:N_EXP] + extra[:, N_EXP : 2 * N_EXP] + extra[:, 2 * N_EXP : 3 * N_EXP]
    e = lax.broadcasted_iota(I32, (n, N_EXP), 1)
    routes = routes_ref[...]
    picked0 = jnp.sum(jnp.where(e == routes[:, 0:1], logits, 0.0), axis=1, keepdims=True)
    picked1 = jnp.sum(jnp.where(e == routes[:, 1:2], logits, 0.0), axis=1, keepdims=True)
    w0 = 1.0 / (1.0 + jnp.exp(picked1 - picked0))
    w1 = 1.0 - w0
    y = y_ref[...]
    mix = (w0 * dot(p0, y) + w1 * dot(p1, y)).astype(BF)
    for b in range(blocks):
        out[b, 0:n, :] = mix[:, b * cols : (b + 1) * cols]


def combine(y, routes, tok, up, blocks):
    n = routes.shape[0]
    width = y.shape[1]
    return pl.pallas_call(
        combine_body,
        out_shape=jax.ShapeDtypeStruct((blocks, n + 2 * (n // blocks), width // blocks), BF),
        in_specs=[VM] * 5,
        out_specs=VM,
        compiler_params=params(),
        name="combine",
    )(y, routes, routes.T, tok, up)


def layer_body(ids, got_ref, tok_ref, out):
    blocks, rows, cols = got_ref.shape
    n = tok_ref.shape[0]
    per = n // blocks
    total = got_ref[0].astype(F32)
    for b in range(1, blocks):
        total = total + got_ref[b].astype(F32)
    tok = tok_ref[:, pl.ds(pl.multiple_of(ids[1] * cols, LANES), cols)]
    layer = (tok.astype(F32) + total[0:n]).astype(BF)
    parts = two(total[n : n + per] + total[n + per : n + 2 * per])
    extra = jnp.concatenate([p.astype(F32) for p in parts], axis=0).astype(BF)
    for b in range(blocks):
        out[b, 0:n, :] = layer
        out[b, n : n + 2 * per, :] = extra


def layer_sum(ids, got, tok):
    return pl.pallas_call(
        layer_body,
        out_shape=jax.ShapeDtypeStruct(got.shape, BF),
        in_specs=[SM, VM, VM],
        out_specs=VM,
        compiler_params=params(),
        name="layer_sum",
    )(ids, got, tok)


def final_body(ids, bound_ref, q0, q1, q2, c0, c1, adapter_ref, up_ref, adapted, clipped, grad, gram):
    blocks, rows, cols = q0.shape
    n = up_ref.shape[0]
    per = n // blocks
    up = up_ref[...]
    mine = ids[1] * N_Q + ids[2]
    acc = jnp.zeros((n, cols), F32)
    gl = jnp.zeros((n, n), F32)
    gram[...] = jnp.zeros((n, n), F32)
    for q, shift, first in ((q0, 0, 0), (c0, 2, 0), (c1, 2, blocks // 2), (q1, 3, 0), (q2, 1, 0)):
        where = quarter(ids, shift) * blocks + first
        for b in range(q.shape[0]):
            s = pl.ds(pl.multiple_of((where + b) * cols, LANES), cols)
            block = q[b, 0:n, :]
            acc = acc + jnp.where(mine == where + b, block.astype(F32), 0.0)
            acc = acc + dot(block, adapter_ref[s, :])
            gl = gl + dot(block, block, (((1,), (1,)), ((), ())))
            grad[s, :] = dot(block, up, (((0,), (0,)), ((), ())))
            extra = q[b, n : n + 2 * per, :].astype(F32)
            at = (first + b) * per
            gram[at : at + per, :] += extra[0:per] + extra[per : 2 * per]
    adapted[...] = acc.astype(BF)
    norm = jnp.sqrt(jnp.maximum(jnp.sum(gl * gram[...], keepdims=True), 0.0))
    limit = bound_ref[0]
    factor = limit / jnp.maximum(norm, limit)
    for b in range(N_Q * blocks):
        s = slice(b * cols, (b + 1) * cols)
        clipped[s, :] = (grad[s, :] * factor).astype(BF)


def final(ids, bound, parts, adapter, up):
    n, cols = up.shape
    width = adapter.shape[0]
    return pl.pallas_call(
        final_body,
        out_shape=[jax.ShapeDtypeStruct((n, cols), BF), jax.ShapeDtypeStruct((width, cols), BF)],
        in_specs=[SM, SM] + [VM] * 7,
        out_specs=[VM, VM],
        scratch_shapes=[pltpu.VMEM((width, cols), F32), pltpu.VMEM((n, n), F32)],
        compiler_params=params(),
        name="final",
    )(ids, bound, *parts, adapter, up)


def exchange(value, axis, groups=None):
    return lax.all_to_all(value, axis, split_axis=0, concat_axis=0, tiled=True, axis_index_groups=groups)


def per_device(tokens, routes, router, w_gate, w_up, w_down, adapter, upstream, bound):
    ids = jnp.stack([lax.axis_index(a) for a in ("expert", Z, Y)]).astype(I32)
    n_z = lax.axis_size(Z)
    groups = holders(n_z)
    q_width = tokens.shape[2] // N_Q
    routed = routes[0]
    wg, wu, wd = w_gate[0], w_up[0], w_down[0]
    up = upstream[0]
    tok = exchange(fill(tokens[0], router.T, n_z * N_Q), FFN).reshape(-1, q_width + LANES)
    packed = pack(tok, routed.T)
    x = exchange(packed.reshape(N_EXP, CAP, q_width), "expert").reshape(N_EXP * CAP, q_width)
    a = y_hop(x, 1)
    b = y_hop(x, -1)
    c0 = z_hop(x[:HALF], 1)
    c1 = z_hop(x[HALF:], -1)
    acc = gates(own_body, ids, (x,), wg, wu)
    acc = gates(far_body, ids, (c0, c1), wg, wu, acc)
    hidden, p, m = turn(ids, a, b, wg, wu, wd, acc)
    p = y_hop(p, 1)
    m = y_hop(m, -1)
    d0, d1, own = downs(ids, hidden, wd)
    total = gather_sum(own, p, m, z_hop(d0, 1), z_hop(d1, -1))
    back = exchange(total.reshape(N_EXP, CAP, q_width), "expert").reshape(N_EXP * CAP, q_width)
    sums = combine(back, routed, tok, up, n_z)
    layer = layer_sum(ids, exchange(sums, FFN, groups), tok)
    layer = exchange(layer, FFN, groups)
    half = n_z // 2
    parts = (
        layer,
        y_hop(layer, 1),
        y_hop(layer, -1),
        z_hop(layer[:half], 1),
        z_hop(layer[half:], -1),
    )
    adapted, clipped = final(ids, bound, parts, adapter[0], up)
    return (adapted[None], clipped[None])


def solution(mesh):
    split = Mesh(mesh.devices.reshape(mesh.shape["expert"], 8, 4), ("expert", "ffn_0", "ffn_1"))
    placed = (
        P("expert", FFN, None),
        P("expert", None, None),
        P(),
        P("expert", None, FFN),
        P("expert", None, FFN),
        P("expert", FFN, None),
        P("expert", None, FFN),
        P("expert", None, FFN),
        P("expert"),
    )
    return jax.shard_map(
        per_device,
        mesh=split,
        in_specs=placed,
        out_specs=(P("expert", None, FFN), P("expert", None, FFN)),
        check_vma=False,
    )
```

```python
import jax
import jax.numpy as jnp
from jax import lax
from jax.experimental import pallas as pl
from jax.experimental.pallas import tpu as pltpu
from jax.sharding import Mesh
from jax.sharding import PartitionSpec as P

FFN = ("ffn_0", "ffn_1")
BF = jnp.bfloat16
F32 = jnp.float32
I32 = jnp.int32
CAP = 48
N_EXP = 8


VM = pl.BlockSpec(memory_space=pltpu.VMEM)
SM = pl.BlockSpec(memory_space=pltpu.SMEM)
HB = pl.BlockSpec(memory_space=pltpu.HBM)


def in_hbm(value):
    return pltpu.with_memory_space_constraint(value, pltpu.HBM)


def dot(a, b, dims=(((1,), (0,)), ((), ()))):
    return lax.dot_general(a, b, dims, preferred_element_type=F32)


def params(mib):
    return pltpu.CompilerParams(vmem_limit_bytes=mib * 1024 * 1024)

Z = "ffn_0"
Y = "ffn_1"
N_Q = 4
HALF = N_EXP * CAP // 2
LANES = 128


def ring(n, k):
    return [(i, (i + k) % n) for i in range(n)]


def y_hop(value, k):
    return lax.ppermute(value, Y, ring(N_Q, k))


def z_hop(value, k):
    return lax.ppermute(value, Z, ring(lax.axis_size(Z), k))


def two(v):
    hi = v.astype(BF)
    return hi, (v - hi.astype(F32)).astype(BF)


def three(v):
    hi = v.astype(BF)
    return (hi, *two(v - hi.astype(F32)))


def quarter(ids, shift):
    return (ids[2] + 2 * (ids[1] & 1) + shift) & (N_Q - 1)


def holders(n_z):
    return [[z * N_Q + (q + 2 * (z % 2)) % N_Q for z in range(n_z)] for q in range(N_Q)]


def hits_of(routes_t):
    n = routes_t.shape[1]
    e = lax.broadcasted_iota(I32, (N_EXP, n), 0)
    return e == routes_t[0:1, :], e == routes_t[1:2, :]


def slot_rows(routes_t):
    n = routes_t.shape[1]
    h0, h1 = hits_of(routes_t)
    hits = (h0 | h1).astype(F32).astype(BF)
    tri = (lax.broadcasted_iota(I32, (n, n), 0) < lax.broadcasted_iota(I32, (n, n), 1)).astype(F32).astype(BF)
    before = dot(hits, tri)
    s0 = jnp.sum(jnp.where(h0, before, 0.0), axis=0, keepdims=True).astype(I32)
    s1 = jnp.sum(jnp.where(h1, before, 0.0), axis=0, keepdims=True).astype(I32)
    return routes_t[0:1, :] * CAP + s0, routes_t[1:2, :] * CAP + s1


def column(row):
    n = row.shape[1]
    diag = lax.broadcasted_iota(I32, (n, n), 0) == lax.broadcasted_iota(I32, (n, n), 1)
    return jnp.sum(jnp.where(diag, jnp.broadcast_to(row.astype(F32), (n, n)), 0.0), axis=1, keepdims=True)


def fill_body(tok_hbm, router_hbm, routes_hbm, out, rows_out, tok_v, router_v, routes_v, sem):
    copies = [
        pltpu.make_async_copy(a, b, sem.at[i])
        for i, (a, b) in enumerate(((tok_hbm, tok_v), (router_hbm, router_v), (routes_hbm, routes_v)))
    ]
    for c in copies:
        c.start()
    dests, mine, full = out.shape
    width = full - LANES
    copies[0].wait()
    tok = tok_v[...]
    for d in range(dests):
        q = (d % N_Q + 2 * (d // N_Q % 2)) % N_Q
        out[d, :, 0:width] = tok[:, q * width : (q + 1) * width]
    copies[2].wait()
    row0, row1 = slot_rows(routes_v[...])
    rows_out[0:1, :] = row0
    rows_out[1:2, :] = row1
    copies[1].wait()
    logits = dot(tok, router_v[...], (((1,), (1,)), ((), ())))
    parts = [p.astype(F32) for p in three(logits)]
    extra = jnp.concatenate(parts + [jnp.zeros((mine, LANES - 3 * N_EXP), F32)], axis=1).astype(BF)
    for d in range(dests):
        out[d, :, width:] = extra


def fill(tok, router_t, routes_t, dests):
    mine, full = tok.shape
    return pl.pallas_call(
        fill_body,
        out_shape=[
            jax.ShapeDtypeStruct((dests, mine, full // N_Q + LANES), BF),
            jax.ShapeDtypeStruct((8, routes_t.shape[1]), I32),
        ],
        in_specs=[HB, HB, HB],
        out_specs=[VM, VM],
        scratch_shapes=[
            pltpu.VMEM(tok.shape, BF),
            pltpu.VMEM(router_t.shape, BF),
            pltpu.VMEM(routes_t.shape, I32),
            pltpu.SemaphoreType.DMA((3,)),
        ],
        compiler_params=params(4),
        name="fill",
    )(in_hbm(tok), in_hbm(router_t), in_hbm(routes_t))


def pack_body(tok_ref, rows_ref, out):
    n = tok_ref.shape[0]
    r = lax.broadcasted_iota(I32, (N_EXP * CAP, n), 0)
    sel = ((r == rows_ref[0:1, :]) | (r == rows_ref[1:2, :])).astype(F32).astype(BF)
    out[...] = dot(sel, tok_ref[:, 0 : out.shape[1]]).astype(BF)


def pack(tok, rows):
    return pl.pallas_call(
        pack_body,
        out_shape=jax.ShapeDtypeStruct((N_EXP * CAP, tok.shape[1] - LANES), BF),
        in_specs=[VM, VM],
        out_specs=VM,
        compiler_params=params(6),
        name="pack",
    )(tok, rows)


def gate_steps(ids, shifts, wg, wu, vg, vu, sem):
    width = vg.shape[1]
    started = []
    for i, shift in enumerate(shifts):
        rows = pl.ds(pl.multiple_of(quarter(ids, shift) * width, LANES), width)
        copies = [
            pltpu.make_async_copy(wg.at[rows], vg.at[i], sem.at[2 * i]),
            pltpu.make_async_copy(wu.at[rows], vu.at[i], sem.at[2 * i + 1]),
        ]
        for c in copies:
            c.start()
        started.append(copies)

    def finish(i, x):
        for c in started[i]:
            c.wait()
        return dot(x, vg[i]), dot(x, vu[i])

    return finish


def gate_scratch(n, width, units):
    return [
        pltpu.VMEM((n, width, units), BF),
        pltpu.VMEM((n, width, units), BF),
        pltpu.SemaphoreType.DMA((2 * n,)),
    ]


def flops(n, width, units):
    work = 4 * n * N_EXP * CAP * width * units
    return pl.CostEstimate(flops=work, bytes_accessed=4 * n * width * units, transcendentals=0)


def own_body(ids, x, wg, wu, out_g, out_u, vg, vu, sem):
    finish = gate_steps(ids, (0,), wg, wu, vg, vu, sem)
    out_g[...], out_u[...] = finish(0, x[...])


def far_body(ids, c0, c1, wg, wu, in_g, in_u, out_g, out_u, vg, vu, sem):
    finish = gate_steps(ids, (2,), wg, wu, vg, vu, sem)
    g, u = finish(0, jnp.concatenate([c0[...], c1[...]], axis=0))
    out_g[...] = in_g[...] + g
    out_u[...] = in_u[...] + u


def gates(body, ids, pieces, wg, wu, acc=()):
    width = pieces[0].shape[1]
    units = wg.shape[1]
    out = jax.ShapeDtypeStruct((N_EXP * CAP, units), F32)
    return pl.pallas_call(
        body,
        out_shape=[out, out],
        in_specs=[SM] + [VM] * len(pieces) + [HB, HB] + [VM] * len(acc),
        out_specs=[VM, VM],
        scratch_shapes=gate_scratch(1, width, units),
        compiler_params=params(10),
        cost_estimate=flops(1, width, units),
        name="gates",
    )(ids, *pieces, wg, wu, *acc)


def start_downs(ids, shifts, wd, vd, sem):
    width = vd.shape[2]
    copies = []
    for i, shift in enumerate(shifts):
        cols = pl.ds(pl.multiple_of(quarter(ids, shift) * width, LANES), width)
        copies.append(pltpu.make_async_copy(wd.at[:, cols], vd.at[i], sem.at[i]))
        copies[-1].start()
    return copies


def turn_body(ids, a, b, wg, wu, wd, in_g, in_u, hidden_ref, out0, out1, vg, vu, sem, vd, sem_d):
    finish = gate_steps(ids, (3, 1), wg, wu, vg, vu, sem)
    copies = start_downs(ids, (1, 3), wd, vd, sem_d)
    g0, u0 = finish(0, a[...])
    g1, u1 = finish(1, b[...])
    g = in_g[...] + g0 + g1
    u = in_u[...] + u0 + u1
    hidden = (g / (1.0 + jnp.exp(-g)) * u).astype(BF)
    hidden_ref[...] = hidden
    for i, out in enumerate((out0, out1)):
        copies[i].wait()
        out[...] = dot(hidden, vd[i]).astype(BF)


def turn(ids, a, b, wg, wu, wd, acc):
    rows, width = a.shape
    units = wg.shape[1]
    out = jax.ShapeDtypeStruct((rows, width), BF)
    return pl.pallas_call(
        turn_body,
        out_shape=[jax.ShapeDtypeStruct((rows, units), BF), out, out],
        in_specs=[SM, VM, VM, HB, HB, HB, VM, VM],
        out_specs=[VM, VM, VM],
        scratch_shapes=gate_scratch(2, width, units)
        + [pltpu.VMEM((2, units, width), BF), pltpu.SemaphoreType.DMA((2,))],
        compiler_params=params(18),
        cost_estimate=flops(3, width, units),
        name="turn",
    )(ids, a, b, wg, wu, wd, *acc)


def downs_body(ids, hidden_ref, wd, out0, out1, own, vd, sem):
    copies = start_downs(ids, (2, 0), wd, vd, sem)
    copies[0].wait()
    y = dot(hidden_ref[...], vd[0]).astype(BF)
    out0[...] = y[:HALF]
    out1[...] = y[HALF:]
    copies[1].wait()
    own[...] = dot(hidden_ref[...], vd[1]).astype(BF)


def downs(ids, hidden, wd):
    units, full = wd.shape
    width = full // N_Q
    half = jax.ShapeDtypeStruct((HALF, width), BF)
    return pl.pallas_call(
        downs_body,
        out_shape=[half, half, jax.ShapeDtypeStruct((2 * HALF, width), BF)],
        in_specs=[SM, VM, HB],
        out_specs=[VM] * 3,
        scratch_shapes=[pltpu.VMEM((2, units, width), BF), pltpu.SemaphoreType.DMA((2,))],
        compiler_params=params(10),
        cost_estimate=flops(1, width, units),
        name="downs",
    )(ids, hidden, wd)


def gather_sum_body(o, a, b, c0, c1, out):
    for s, c in ((slice(0, HALF), c0), (slice(HALF, 2 * HALF), c1)):
        out[s, :] = (o[s, :].astype(F32) + a[s, :].astype(F32) + b[s, :].astype(F32) + c[...].astype(F32)).astype(BF)


def gather_sum(*args):
    return pl.pallas_call(
        gather_sum_body,
        out_shape=jax.ShapeDtypeStruct(args[0].shape, BF),
        in_specs=[VM] * 5,
        out_specs=VM,
        compiler_params=params(8),
        name="gather_sum",
    )(*args)


def combine_body(y_ref, rows_ref, tok_ref, up_ref, out):
    blocks, _, cols = out.shape
    up = up_ref[...]
    n = up.shape[0]
    per = n // blocks
    gram = [p.astype(F32) for p in two(dot(up, up, (((1,), (1,)), ((), ()))))]
    for b in range(blocks):
        s = slice(b * per, (b + 1) * per)
        out[b, n : n + 2 * per, :] = jnp.concatenate([g[s] for g in gram], axis=0).astype(BF)
    row0 = column(rows_ref[0:1, :])
    row1 = column(rows_ref[1:2, :])
    r = lax.broadcasted_iota(I32, (n, N_EXP * CAP), 1).astype(F32)
    p0 = (r == row0).astype(F32).astype(BF)
    p1 = (r == row1).astype(F32).astype(BF)
    extra = tok_ref[:, y_ref.shape[1] :].astype(F32)
    logits = extra[:, 0:N_EXP] + extra[:, N_EXP : 2 * N_EXP] + extra[:, 2 * N_EXP : 3 * N_EXP]
    e = (lax.broadcasted_iota(I32, (n, N_EXP), 1) * CAP).astype(F32)
    picked0 = jnp.sum(jnp.where((row0 >= e) & (row0 < e + CAP), logits, 0.0), axis=1, keepdims=True)
    picked1 = jnp.sum(jnp.where((row1 >= e) & (row1 < e + CAP), logits, 0.0), axis=1, keepdims=True)
    w0 = 1.0 / (1.0 + jnp.exp(picked1 - picked0))
    w1 = 1.0 - w0
    y = y_ref[...]
    mix = (w0 * dot(p0, y) + w1 * dot(p1, y)).astype(BF)
    for b in range(blocks):
        out[b, 0:n, :] = mix[:, b * cols : (b + 1) * cols]


def combine(y, rows, tok, up, blocks):
    n = tok.shape[0]
    width = y.shape[1]
    return pl.pallas_call(
        combine_body,
        out_shape=jax.ShapeDtypeStruct((blocks, n + 2 * (n // blocks), width // blocks), BF),
        in_specs=[VM] * 4,
        out_specs=VM,
        compiler_params=params(10),
        name="combine",
    )(y, rows, tok, up)


def layer_body(ids, got_ref, tok_ref, out):
    blocks, rows, cols = got_ref.shape
    n = tok_ref.shape[0]
    per = n // blocks
    total = got_ref[0].astype(F32)
    for b in range(1, blocks):
        total = total + got_ref[b].astype(F32)
    tok = tok_ref[:, pl.ds(pl.multiple_of(ids[1] * cols, LANES), cols)]
    layer = (tok.astype(F32) + total[0:n]).astype(BF)
    parts = two(total[n : n + per] + total[n + per : n + 2 * per])
    extra = jnp.concatenate([p.astype(F32) for p in parts], axis=0).astype(BF)
    for b in range(blocks):
        out[b, 0:n, :] = layer
        out[b, n : n + 2 * per, :] = extra


def layer_sum(ids, got, tok):
    return pl.pallas_call(
        layer_body,
        out_shape=jax.ShapeDtypeStruct(got.shape, BF),
        in_specs=[SM, VM, VM],
        out_specs=VM,
        compiler_params=params(6),
        name="layer_sum",
    )(ids, got, tok)


def final_body(ids, bound_ref, q0, q1, q2, q3, adapter_ref, up_ref, adapted, clipped, grad, gram):
    blocks, rows, cols = q0.shape
    n = up_ref.shape[0]
    per = n // blocks
    up = up_ref[...]
    mine = ids[1] * N_Q + ids[2]
    acc = jnp.zeros((n, cols), F32)
    gl = jnp.zeros((n, n), F32)
    gram[...] = jnp.zeros((n, n), F32)
    for q, shift in ((q0, 0), (q1, 3), (q2, 1), (q3, 2)):
        where = quarter(ids, shift) * blocks
        for b in range(blocks):
            s = pl.ds(pl.multiple_of((where + b) * cols, LANES), cols)
            block = q[b, 0:n, :]
            acc = acc + jnp.where(mine == where + b, block.astype(F32), 0.0)
            acc = acc + dot(block, adapter_ref[s, :])
            gl = gl + dot(block, block, (((1,), (1,)), ((), ())))
            grad[s, :] = dot(block, up, (((0,), (0,)), ((), ())))
            extra = q[b, n : n + 2 * per, :].astype(F32)
            gram[b * per : (b + 1) * per, :] += extra[0:per] + extra[per : 2 * per]
    adapted[...] = acc.astype(BF)
    norm = jnp.sqrt(jnp.maximum(jnp.sum(gl * gram[...], keepdims=True), 0.0))
    limit = bound_ref[0]
    factor = limit / jnp.maximum(norm, limit)
    for b in range(N_Q * blocks):
        s = slice(b * cols, (b + 1) * cols)
        clipped[s, :] = (grad[s, :] * factor).astype(BF)


def final(ids, bound, parts, adapter, up):
    n, cols = up.shape
    width = adapter.shape[0]
    return pl.pallas_call(
        final_body,
        out_shape=[jax.ShapeDtypeStruct((n, cols), BF), jax.ShapeDtypeStruct((width, cols), BF)],
        in_specs=[SM, SM] + [VM] * 6,
        out_specs=[VM, VM],
        scratch_shapes=[pltpu.VMEM((width, cols), F32), pltpu.VMEM((n, n), F32)],
        compiler_params=params(14),
        name="final",
    )(ids, bound, *parts, adapter, up)


def exchange(value, axis, groups=None):
    return lax.all_to_all(value, axis, split_axis=0, concat_axis=0, tiled=True, axis_index_groups=groups)


def per_device(tokens, routes, router, w_gate, w_up, w_down, adapter, upstream, bound):
    ids = jnp.stack([lax.axis_index(a) for a in ("expert", Z, Y)]).astype(I32)
    n_z = lax.axis_size(Z)
    groups = holders(n_z)
    q_width = tokens.shape[2] // N_Q
    wg, wu, wd = (in_hbm(w[0]) for w in (w_gate, w_up, w_down))
    up = upstream[0]
    outgoing, rows = fill(tokens[0], router.T, routes[0].T, n_z * N_Q)
    tok = exchange(outgoing, FFN).reshape(-1, q_width + LANES)
    packed = pack(tok, rows)
    x = exchange(packed.reshape(N_EXP, CAP, q_width), "expert").reshape(N_EXP * CAP, q_width)
    a = y_hop(x, 1)
    b = y_hop(x, -1)
    c0 = z_hop(x[:HALF], 1)
    c1 = z_hop(x[HALF:], -1)
    acc = gates(own_body, ids, (x,), wg, wu)
    acc = gates(far_body, ids, (c0, c1), wg, wu, acc)
    hidden, p, m = turn(ids, a, b, wg, wu, wd, acc)
    p = y_hop(p, 1)
    m = y_hop(m, -1)
    d0, d1, own = downs(ids, hidden, wd)
    total = gather_sum(own, p, m, z_hop(d0, 1), z_hop(d1, -1))
    back = exchange(total.reshape(N_EXP, CAP, q_width), "expert").reshape(N_EXP * CAP, q_width)
    sums = combine(back, rows, tok, up, n_z)
    layer = layer_sum(ids, exchange(sums, FFN, groups), tok)
    layer = exchange(layer, FFN, groups)
    parts = (layer, y_hop(layer, 1), y_hop(layer, -1), z_hop(layer, 1))
    adapted, clipped = final(ids, bound, parts, adapter[0], up)
    return (adapted[None], clipped[None])


def solution(mesh):
    split = Mesh(mesh.devices.reshape(mesh.shape["expert"], 8, 4), ("expert", "ffn_0", "ffn_1"))
    placed = (
        P("expert", FFN, None),
        P("expert", None, None),
        P(),
        P("expert", None, FFN),
        P("expert", None, FFN),
        P("expert", FFN, None),
        P("expert", None, FFN),
        P("expert", None, FFN),
        P("expert"),
    )
    return jax.shard_map(
        per_device,
        mesh=split,
        in_specs=placed,
        out_specs=(P("expert", None, FFN), P("expert", None, FFN)),
        check_vma=False,
    )
```

```python
import jax
import jax.numpy as jnp
from jax import lax
from jax.experimental import pallas as pl
from jax.experimental.pallas import tpu as pltpu
from jax.sharding import Mesh
from jax.sharding import PartitionSpec as P

FFN = ("ffn_0", "ffn_1")
BF = jnp.bfloat16
F32 = jnp.float32
I32 = jnp.int32
CAP = 48
N_EXP = 8


VM = pl.BlockSpec(memory_space=pltpu.VMEM)
SM = pl.BlockSpec(memory_space=pltpu.SMEM)
HB = pl.BlockSpec(memory_space=pltpu.HBM)


def in_hbm(value):
    return pltpu.with_memory_space_constraint(value, pltpu.HBM)


def dot(a, b, dims=(((1,), (0,)), ((), ()))):
    return lax.dot_general(a, b, dims, preferred_element_type=F32)


def params(mib):
    return pltpu.CompilerParams(vmem_limit_bytes=mib * 1024 * 1024)

Z = "ffn_0"
Y = "ffn_1"
N_Q = 4
HALF = N_EXP * CAP // 2
LANES = 128


def ring(n, k):
    return [(i, (i + k) % n) for i in range(n)]


def y_hop(value, k):
    return lax.ppermute(value, Y, ring(N_Q, k))


def z_hop(value, k):
    return lax.ppermute(value, Z, ring(lax.axis_size(Z), k))


def two(v):
    hi = v.astype(BF)
    return hi, (v - hi.astype(F32)).astype(BF)


def three(v):
    hi = v.astype(BF)
    return (hi, *two(v - hi.astype(F32)))


def quarter(ids, shift):
    return (ids[2] + 2 * (ids[1] & 1) + shift) & (N_Q - 1)


def holders(n_z):
    return [[z * N_Q + (q + 2 * (z % 2)) % N_Q for z in range(n_z)] for q in range(N_Q)]


def hits_of(routes_t):
    n = routes_t.shape[1]
    e = lax.broadcasted_iota(I32, (N_EXP, n), 0)
    return e == routes_t[0:1, :], e == routes_t[1:2, :]


def slot_rows(routes_t):
    n = routes_t.shape[1]
    h0, h1 = hits_of(routes_t)
    hits = (h0 | h1).astype(F32).astype(BF)
    tri = (lax.broadcasted_iota(I32, (n, n), 0) < lax.broadcasted_iota(I32, (n, n), 1)).astype(F32).astype(BF)
    before = dot(hits, tri)
    s0 = jnp.sum(jnp.where(h0, before, 0.0), axis=0, keepdims=True).astype(I32)
    s1 = jnp.sum(jnp.where(h1, before, 0.0), axis=0, keepdims=True).astype(I32)
    return routes_t[0:1, :] * CAP + s0, routes_t[1:2, :] * CAP + s1


def column(row):
    n = row.shape[1]
    diag = lax.broadcasted_iota(I32, (n, n), 0) == lax.broadcasted_iota(I32, (n, n), 1)
    return jnp.sum(jnp.where(diag, jnp.broadcast_to(row.astype(F32), (n, n)), 0.0), axis=1, keepdims=True)


def fill_body(tok_hbm, router_hbm, routes_hbm, out, rows_out, tok_v, router_v, routes_v, sem):
    copies = [
        pltpu.make_async_copy(a, b, sem.at[i])
        for i, (a, b) in enumerate(((tok_hbm, tok_v), (router_hbm, router_v), (routes_hbm, routes_v)))
    ]
    for c in copies:
        c.start()
    dests, mine, full = out.shape
    width = full - LANES
    copies[0].wait()
    tok = tok_v[...]
    for d in range(dests):
        q = (d % N_Q + 2 * (d // N_Q % 2)) % N_Q
        out[d, :, 0:width] = tok[:, q * width : (q + 1) * width]
    copies[2].wait()
    row0, row1 = slot_rows(routes_v[...])
    rows_out[0:1, :] = row0
    rows_out[1:2, :] = row1
    copies[1].wait()
    logits = dot(tok, router_v[...], (((1,), (1,)), ((), ())))
    parts = [p.astype(F32) for p in three(logits)]
    extra = jnp.concatenate(parts + [jnp.zeros((mine, LANES - 3 * N_EXP), F32)], axis=1).astype(BF)
    for d in range(dests):
        out[d, :, width:] = extra


def fill(tok, router_t, routes_t, dests):
    mine, full = tok.shape
    return pl.pallas_call(
        fill_body,
        out_shape=[
            jax.ShapeDtypeStruct((dests, mine, full // N_Q + LANES), BF),
            jax.ShapeDtypeStruct((8, routes_t.shape[1]), I32),
        ],
        in_specs=[HB, HB, HB],
        out_specs=[VM, VM],
        scratch_shapes=[
            pltpu.VMEM(tok.shape, BF),
            pltpu.VMEM(router_t.shape, BF),
            pltpu.VMEM(routes_t.shape, I32),
            pltpu.SemaphoreType.DMA((3,)),
        ],
        compiler_params=params(4),
        name="fill",
    )(in_hbm(tok), in_hbm(router_t), in_hbm(routes_t))


def pack_body(tok_ref, rows_ref, out):
    n = tok_ref.shape[0]
    r = lax.broadcasted_iota(I32, (N_EXP * CAP, n), 0)
    sel = ((r == rows_ref[0:1, :]) | (r == rows_ref[1:2, :])).astype(F32).astype(BF)
    out[...] = dot(sel, tok_ref[:, 0 : out.shape[1]]).astype(BF)


def pack(tok, rows):
    return pl.pallas_call(
        pack_body,
        out_shape=jax.ShapeDtypeStruct((N_EXP * CAP, tok.shape[1] - LANES), BF),
        in_specs=[VM, VM],
        out_specs=VM,
        compiler_params=params(6),
        name="pack",
    )(tok, rows)


def halve_body(x, out0, out1):
    out0[...] = x[0:HALF, :]
    out1[...] = x[HALF:, :]


def halve(x):
    half = jax.ShapeDtypeStruct((HALF, x.shape[1]), BF)
    return pl.pallas_call(
        halve_body,
        out_shape=[half, half],
        in_specs=[VM],
        out_specs=[VM, VM],
        compiler_params=params(6),
        name="halve",
    )(x)


def gate_copies(ids, shift, wg, wu, out, sems):
    width = out.shape[0]
    units = wg.shape[1]
    rows = pl.ds(pl.multiple_of(quarter(ids, shift) * width, LANES), width)
    return [
        pltpu.make_async_copy(wg.at[rows], out.at[:, pl.ds(0, units)], sems[0]),
        pltpu.make_async_copy(wu.at[rows], out.at[:, pl.ds(units, units)], sems[1]),
    ]


def own_body(ids, h0, h1, wg, wu, wd, acc, w_next, w_down, v, sem):
    width = v.shape[0]
    copies = gate_copies(ids, 0, wg, wu, v, (sem.at[0], sem.at[1]))
    for i, shift in enumerate((3, 1)):
        copies += gate_copies(ids, shift, wg, wu, w_next.at[i], (sem.at[2 + 2 * i], sem.at[3 + 2 * i]))
    for i, shift in enumerate((1, 3, 2, 0)):
        cols = pl.ds(pl.multiple_of(quarter(ids, shift) * width, LANES), width)
        copies.append(pltpu.make_async_copy(wd.at[:, cols], w_down.at[i], sem.at[6 + i]))
    for c in copies:
        c.start()
    copies[0].wait()
    copies[1].wait()
    acc[0:HALF, :] = dot(h0[...], v[...])
    acc[HALF:, :] = dot(h1[...], v[...])
    for c in copies[2:]:
        c.wait()


def own_gates(ids, h0, h1, wg, wu, wd):
    width = h0.shape[1]
    units = wg.shape[1]
    return pl.pallas_call(
        own_body,
        out_shape=[
            jax.ShapeDtypeStruct((2 * HALF, 2 * units), F32),
            jax.ShapeDtypeStruct((2, width, 2 * units), BF),
            jax.ShapeDtypeStruct((N_Q, units, width), BF),
        ],
        in_specs=[SM, VM, VM, HB, HB, HB],
        out_specs=[VM] * 3,
        scratch_shapes=[pltpu.VMEM((width, 2 * units), BF), pltpu.SemaphoreType.DMA((10,))],
        compiler_params=params(16),
        cost_estimate=flops(1, width, units),
        name="own_gates",
    )(ids, h0, h1, wg, wu, wd)


def far_body(ids, c0, c1, wg, wu, acc, out, v, sem):
    copies = gate_copies(ids, 2, wg, wu, v, (sem.at[0], sem.at[1]))
    for c in copies:
        c.start()
    for c in copies:
        c.wait()
    out[0:HALF, :] = acc[0:HALF, :] + dot(c0[...], v[...])
    out[HALF:, :] = acc[HALF:, :] + dot(c1[...], v[...])


def far_gates(ids, c0, c1, wg, wu, acc):
    width = c0.shape[1]
    units = wg.shape[1]
    return pl.pallas_call(
        far_body,
        out_shape=jax.ShapeDtypeStruct(acc.shape, F32),
        in_specs=[SM, VM, VM, HB, HB, VM],
        out_specs=VM,
        scratch_shapes=[pltpu.VMEM((width, 2 * units), BF), pltpu.SemaphoreType.DMA((2,))],
        compiler_params=params(10),
        cost_estimate=flops(1, width, units),
        name="far_gates",
    )(ids, c0, c1, wg, wu, acc)


def flops(n, width, units):
    work = 4 * n * N_EXP * CAP * width * units
    return pl.CostEstimate(flops=work, bytes_accessed=4 * n * width * units, transcendentals=0)


def turn(a, b, acc, w_next, w_down, part):
    rows, width = a.shape
    units = w_down.shape[1]
    out = jax.ShapeDtypeStruct((rows, width), BF)

    def body(a, b, acc, w_next, w_down, hidden_ref, out0, out1):
        both = acc[part * rows : (part + 1) * rows, :] + dot(a[...], w_next[0]) + dot(b[...], w_next[1])
        g = both[:, :units]
        hidden = (g / (1.0 + jnp.exp(-g)) * both[:, units:]).astype(BF)
        hidden_ref[...] = hidden
        out0[...] = dot(hidden, w_down[0]).astype(BF)
        out1[...] = dot(hidden, w_down[1]).astype(BF)

    return pl.pallas_call(
        body,
        out_shape=[jax.ShapeDtypeStruct((rows, units), BF), out, out],
        in_specs=[VM] * 5,
        out_specs=[VM] * 3,
        compiler_params=params(14),
        cost_estimate=flops(1, width, units),
        name=f"turn{part}",
    )(a, b, acc, w_next, w_down)


def downs_body(hidden_ref, w_down, far, own):
    hidden = hidden_ref[...]
    far[...] = dot(hidden, w_down[2]).astype(BF)
    own[...] = dot(hidden, w_down[3]).astype(BF)


def downs(hidden, w_down):
    rows, units = hidden.shape
    out = jax.ShapeDtypeStruct((rows, w_down.shape[2]), BF)
    return pl.pallas_call(
        downs_body,
        out_shape=[out, out],
        in_specs=[VM, VM],
        out_specs=[VM, VM],
        compiler_params=params(10),
        cost_estimate=flops(1, w_down.shape[2], units // 2),
        name="downs",
    )(hidden, w_down)


def gather_sum_body(*refs):
    out = refs[-1]
    for part in range(2):
        total = sum(r[...].astype(F32) for r in refs[4 * part : 4 * part + 4])
        out[part * HALF : (part + 1) * HALF, :] = total.astype(BF)


def gather_sum(*args):
    return pl.pallas_call(
        gather_sum_body,
        out_shape=jax.ShapeDtypeStruct((2 * HALF, args[0].shape[1]), BF),
        in_specs=[VM] * 8,
        out_specs=VM,
        compiler_params=params(8),
        name="gather_sum",
    )(*args)


def combine_body(y_ref, rows_ref, tok_ref, up_ref, out):
    blocks, _, cols = out.shape
    up = up_ref[...]
    n = up.shape[0]
    per = n // blocks
    gram = [p.astype(F32) for p in two(dot(up, up, (((1,), (1,)), ((), ()))))]
    for b in range(blocks):
        s = slice(b * per, (b + 1) * per)
        out[b, n : n + 2 * per, :] = jnp.concatenate([g[s] for g in gram], axis=0).astype(BF)
    row0 = column(rows_ref[0:1, :])
    row1 = column(rows_ref[1:2, :])
    r = lax.broadcasted_iota(I32, (n, N_EXP * CAP), 1).astype(F32)
    p0 = (r == row0).astype(F32).astype(BF)
    p1 = (r == row1).astype(F32).astype(BF)
    extra = tok_ref[:, y_ref.shape[1] :].astype(F32)
    logits = extra[:, 0:N_EXP] + extra[:, N_EXP : 2 * N_EXP] + extra[:, 2 * N_EXP : 3 * N_EXP]
    e = (lax.broadcasted_iota(I32, (n, N_EXP), 1) * CAP).astype(F32)
    picked0 = jnp.sum(jnp.where((row0 >= e) & (row0 < e + CAP), logits, 0.0), axis=1, keepdims=True)
    picked1 = jnp.sum(jnp.where((row1 >= e) & (row1 < e + CAP), logits, 0.0), axis=1, keepdims=True)
    w0 = 1.0 / (1.0 + jnp.exp(picked1 - picked0))
    w1 = 1.0 - w0
    y = y_ref[...]
    mix = (w0 * dot(p0, y) + w1 * dot(p1, y)).astype(BF)
    for b in range(blocks):
        out[b, 0:n, :] = mix[:, b * cols : (b + 1) * cols]


def combine(y, rows, tok, up, blocks):
    n = tok.shape[0]
    width = y.shape[1]
    return pl.pallas_call(
        combine_body,
        out_shape=jax.ShapeDtypeStruct((blocks, n + 2 * (n // blocks), width // blocks), BF),
        in_specs=[VM] * 4,
        out_specs=VM,
        compiler_params=params(10),
        name="combine",
    )(y, rows, tok, up)


def layer_body(ids, got_ref, tok_ref, out):
    blocks, rows, cols = got_ref.shape
    n = tok_ref.shape[0]
    per = n // blocks
    total = got_ref[0].astype(F32)
    for b in range(1, blocks):
        total = total + got_ref[b].astype(F32)
    tok = tok_ref[:, pl.ds(pl.multiple_of(ids[1] * cols, LANES), cols)]
    layer = (tok.astype(F32) + total[0:n]).astype(BF)
    parts = two(total[n : n + per] + total[n + per : n + 2 * per])
    extra = jnp.concatenate([p.astype(F32) for p in parts], axis=0).astype(BF)
    for b in range(blocks):
        out[b, 0:n, :] = layer
        out[b, n : n + 2 * per, :] = extra


def layer_sum(ids, got, tok):
    return pl.pallas_call(
        layer_body,
        out_shape=jax.ShapeDtypeStruct(got.shape, BF),
        in_specs=[SM, VM, VM],
        out_specs=VM,
        compiler_params=params(6),
        name="layer_sum",
    )(ids, got, tok)


def final_body(ids, bound_ref, q0, q1, q2, q3, adapter_ref, up_ref, adapted, clipped, grad, gram):
    blocks, rows, cols = q0.shape
    n = up_ref.shape[0]
    per = n // blocks
    up = up_ref[...]
    mine = ids[1] * N_Q + ids[2]
    acc = jnp.zeros((n, cols), F32)
    gl = jnp.zeros((n, n), F32)
    gram[...] = jnp.zeros((n, n), F32)
    for q, shift in ((q0, 0), (q1, 3), (q2, 1), (q3, 2)):
        where = quarter(ids, shift)
        own = q[lax.rem(mine, blocks), 0:n, :].astype(F32)
        acc = acc + jnp.where(lax.div(mine, blocks) == where, own, 0.0)
        whole = jnp.concatenate([q[b, 0:n, :] for b in range(blocks)], axis=1)
        s = pl.ds(pl.multiple_of(where * blocks * cols, LANES), blocks * cols)
        acc = acc + dot(whole, adapter_ref[s, :])
        gl = gl + dot(whole, whole, (((1,), (1,)), ((), ())))
        grad[s, :] = dot(whole, up, (((0,), (0,)), ((), ())))
        for b in range(blocks):
            extra = q[b, n : n + 2 * per, :].astype(F32)
            gram[b * per : (b + 1) * per, :] += extra[0:per] + extra[per : 2 * per]
    adapted[...] = acc.astype(BF)
    norm = jnp.sqrt(jnp.maximum(jnp.sum(gl * gram[...], keepdims=True), 0.0))
    limit = bound_ref[0]
    factor = limit / jnp.maximum(norm, limit)
    for b in range(N_Q * blocks):
        s = slice(b * cols, (b + 1) * cols)
        clipped[s, :] = (grad[s, :] * factor).astype(BF)


def final(ids, bound, parts, adapter, up):
    n, cols = up.shape
    width = adapter.shape[0]
    return pl.pallas_call(
        final_body,
        out_shape=[jax.ShapeDtypeStruct((n, cols), BF), jax.ShapeDtypeStruct((width, cols), BF)],
        in_specs=[SM, SM] + [VM] * 6,
        out_specs=[VM, VM],
        scratch_shapes=[pltpu.VMEM((width, cols), F32), pltpu.VMEM((n, n), F32)],
        compiler_params=params(14),
        name="final",
    )(ids, bound, *parts, adapter, up)


def exchange(value, axis, groups=None):
    return lax.all_to_all(value, axis, split_axis=0, concat_axis=0, tiled=True, axis_index_groups=groups)


def per_device(tokens, routes, router, w_gate, w_up, w_down, adapter, upstream, bound):
    ids = jnp.stack([lax.axis_index(a) for a in ("expert", Z, Y)]).astype(I32)
    n_z = lax.axis_size(Z)
    groups = holders(n_z)
    q_width = tokens.shape[2] // N_Q
    wg, wu, wd = (in_hbm(w[0]) for w in (w_gate, w_up, w_down))
    up = upstream[0]
    outgoing, rows = fill(tokens[0], router.T, routes[0].T, n_z * N_Q)
    tok = exchange(outgoing, FFN).reshape(-1, q_width + LANES)
    packed = pack(tok, rows)
    x = exchange(packed.reshape(N_EXP, CAP, q_width), "expert").reshape(N_EXP * CAP, q_width)
    h0, h1 = halve(x)
    a0, b0, c0 = y_hop(h0, 1), y_hop(h0, -1), z_hop(h0, 1)
    a1, b1, c1 = y_hop(h1, 1), y_hop(h1, -1), z_hop(h1, -1)
    acc, w_next, w_down4 = own_gates(ids, h0, h1, wg, wu, wd)
    acc = far_gates(ids, c0, c1, wg, wu, acc)
    hidden0, p0, m0 = turn(a0, b0, acc, w_next, w_down4, 0)
    p0, m0 = y_hop(p0, 1), y_hop(m0, -1)
    d0, o0 = downs(hidden0, w_down4)
    d0 = z_hop(d0, 1)
    hidden1, p1, m1 = turn(a1, b1, acc, w_next, w_down4, 1)
    p1, m1 = y_hop(p1, 1), y_hop(m1, -1)
    d1, o1 = downs(hidden1, w_down4)
    d1 = z_hop(d1, -1)
    total = gather_sum(o0, d0, p0, m0, o1, d1, p1, m1)
    back = exchange(total.reshape(N_EXP, CAP, q_width), "expert").reshape(N_EXP * CAP, q_width)
    sums = combine(back, rows, tok, up, n_z)
    layer = layer_sum(ids, exchange(sums, FFN, groups), tok)
    layer = exchange(layer, FFN, groups)
    parts = (layer, y_hop(layer, 1), y_hop(layer, -1), z_hop(layer, 1))
    adapted, clipped = final(ids, bound, parts, adapter[0], up)
    return (adapted[None], clipped[None])


def solution(mesh):
    split = Mesh(mesh.devices.reshape(mesh.shape["expert"], 8, 4), ("expert", "ffn_0", "ffn_1"))
    placed = (
        P("expert", FFN, None),
        P("expert", None, None),
        P(),
        P("expert", None, FFN),
        P("expert", None, FFN),
        P("expert", FFN, None),
        P("expert", None, FFN),
        P("expert", None, FFN),
        P("expert"),
    )
    return jax.shard_map(
        per_device,
        mesh=split,
        in_specs=placed,
        out_specs=(P("expert", None, FFN), P("expert", None, FFN)),
        check_vma=False,
    )
```
